32 devices in a mesh: dp: 16 (over z, y, core), shard: 2 (over x).
Axes of the slice: x: 2, y: 2, z: 4, core: 2. Of those that a mesh axis runs over, the one named last changes fastest.
Arguments:
- hidden: bfloat16 [8192, 2560], P(('dp', 'shard')), may hold values from -6 to 6
- resid: bfloat16 [1280, 8192], P('shard', 'dp'), may hold values from -6 to 6
- target: bfloat16 [1280, 8192], P('shard', 'dp'), may hold values from -6 to 6
- w_out: bfloat16 [1280, 2560], P('shard'), may hold values from -0.125 to 0.125
- signs: int32 [40, 2560], P('shard'), may hold values from -2147483648 to 2147483646
- m_old: float32 [25600, 128], P(('shard', 'dp')), may hold values from -4 to 4
- v_old: float32 [25600, 128], P(('shard', 'dp')), may hold values from 0.8192 to 8.192
Outputs:
- new_w: bfloat16 [1280, 2560], P('shard')
- new_m: float32 [25600, 128], P(('shard', 'dp'))
- new_v: float32 [25600, 128], P(('shard', 'dp'))
The draws below stay inside these ranges and needn't reach their ends.
Inputs may be any that keep to these rules, and one draw needn't show every extreme that they name: Every word carries 32 independent signs, bit b of word k belonging to output feature 32 k + b.
All inputs are finite; a program needn't handle non-finite values.
Results may differ from the reference program's by a relative error of at most 0.0023.
Values may be sent and summed in bfloat16 or wider, within the bound.
A program may use at most 64 MiB of HBM per device.

```python
import math
import jax
import jax.numpy as jnp
from jax import lax

D = 1280
HID = 2560
TOK_DEV = 256
OPT_STEP = 10
TOKENS = 8192
N_DP = 16
N_SHARD = 2


def place_ends(values, stream_key, smallest, top_value):
    spot = [jax.random.randint(jax.random.fold_in(stream_key, axis), (), 0, length) for axis, length in enumerate(values.shape)]
    longest = values.shape.index(max(values.shape))
    beside = spot[:longest] + [(spot[longest] + 1) % values.shape[longest]] + spot[longest + 1:]
    return values.at[tuple(spot)].set(smallest).at[tuple(beside)].set(top_value)


def block_levels(key, dims, pieces, smallest, top_value):
    level = 1.0
    for position, shards_of in pieces:
        draws = jax.random.uniform(jax.random.fold_in(jax.random.fold_in(key, 6), position), (shards_of,), jnp.float32, smallest / len(pieces), top_value / len(pieces))
        level = level * jnp.repeat(jnp.exp(draws), dims[position] // shards_of).reshape((-1,) + (1,) * (len(dims) - 1 - position))
    return level


def noise(key, dims, scale, reach, split=(), kind=jnp.bfloat16):
    gain = block_levels(key, dims, split, -0.22, 0.18) if split else 1.0
    values = jax.random.normal(key, dims, jnp.float32) * scale * gain
    return jnp.minimum(jnp.maximum(values, -reach), reach).astype(kind)


def setup_inputs(seed: int = 0) -> dict:
    splits = jax.random.split(jax.random.key(seed), 8)
    return {
        "hidden": noise(splits[0], (TOKENS, HID), 1.0, 6.0, ((0, 32),)),
        "resid": noise(splits[1], (D, TOKENS), 1.0, 6.0, ((0, 2), (1, 16))),
        "target": noise(splits[2], (D, TOKENS), 1.0, 6.0, ((0, 2), (1, 16))),
        "w_out": noise(splits[3], (D, HID), HID ** -0.5, 0.125, ((0, 2),)),
        "signs": place_ends(jax.random.randint(splits[4], (D // 32, HID), -2147483648, 2147483647), jax.random.fold_in(splits[4], 1), -2147483648, 2147483646).astype(jnp.int32),
        "m_old": noise(splits[5], (D * HID // 128, 128), 0.6, 4.0, ((0, 32),), jnp.float32),
        "v_old": jnp.clip(jnp.exp(math.log(8.192) - 2.3025852 * jax.random.uniform(splits[6], (D * HID // 128, 128), jnp.float32) ** block_levels(splits[6], (D * HID // 128, 128), ((0, 32),), -0.2, 0.2)), 0.8192, 8.192),
    }


def unpack_signs(signs):
    shifts = jnp.arange(32, dtype=jnp.int32)
    bit_values = jnp.bitwise_and(jnp.right_shift(signs[:, None, :], shifts[None, :, None]), 1)
    return (1 - 2 * bit_values).reshape(signs.shape[0] * 32, signs.shape[1]).astype(jnp.bfloat16)

def reference(hidden, resid, target, w_out, signs, m_old, v_old):
    probes = unpack_signs(signs)
    group_size = TOK_DEV * N_SHARD
    blocks = hidden.reshape(N_DP, group_size, HID)
    resid_blocks = jnp.transpose(resid.reshape(D, N_DP, group_size), (1, 0, 2))
    target_blocks = jnp.transpose(target.reshape(D, N_DP, group_size), (1, 0, 2))
    stacked = jnp.concatenate([w_out, probes], axis=0)

    def accumulate(running, block_items):
        hidden_block, resid_block, target_block = block_items
        forward = lax.dot_general(stacked, hidden_block, (((1,), (1,)), ((), ())), preferred_element_type=jnp.float32)
        output = forward[:D]
        tangent = forward[D:]
        misfit = resid_block.astype(jnp.float32) + output - target_block.astype(jnp.float32)
        spread = 1.0 + misfit * misfit
        rooted = jnp.sqrt(spread)
        slopes = (misfit / rooted).astype(jnp.bfloat16)
        bends = (tangent / (spread * rooted)).astype(jnp.bfloat16)
        grad_part = jnp.dot(slopes, hidden_block, preferred_element_type=jnp.float32)
        curve_part = jnp.dot(bends, hidden_block, preferred_element_type=jnp.float32)
        return ((running[0] + grad_part, running[1] + curve_part), None)
    empty = jnp.zeros((D, HID), jnp.float32)
    (grad_sum, curve_sum), _ = lax.scan(accumulate, (empty, empty), (blocks, resid_blocks, target_blocks))
    scaling = 1.0 / math.sqrt(TOKENS)
    gradient = (grad_sum * scaling).reshape(D * HID // 128, 128)
    curvature = (curve_sum * scaling).reshape(D * HID // 128, 128)
    diag_est = probes.astype(jnp.float32).reshape(D * HID // 128, 128) * curvature
    new_m = 0.9 * m_old + 0.1 * gradient
    new_v = 0.999 * v_old + 0.001 * diag_est * diag_est
    first_fix = 1.0 - 0.9 ** OPT_STEP
    second_fix = 1.0 - 0.999 ** OPT_STEP
    update = new_m / first_fix / (jnp.sqrt(new_v / second_fix) + 0.0001)
    new_w = (w_out.astype(jnp.float32) - 0.15 * update.reshape(D, HID)).astype(jnp.bfloat16)
    return (new_w, new_m, new_v)
```

```python
import functools
import math

import jax
import jax.numpy as jnp
from jax import lax
from jax.experimental import pallas as pl
from jax.experimental.pallas import tpu as pltpu
from jax.sharding import PartitionSpec as P

OPT_STEP = 10


beta_one = 0.9
beta_two = 0.999
learn_rate = 0.15
epsilon = 0.0001


def unpack_signs(signs):
    shifts = jnp.arange(32, dtype=jnp.int32)
    bit_values = jnp.bitwise_and(jnp.right_shift(signs[:, None, :], shifts[None, :, None]), 1)
    return (1 - 2 * bit_values).reshape(signs.shape[0] * 32, signs.shape[1]).astype(jnp.bfloat16)


def on_device(hidden, resid, target, w_out, signs, m_old, v_old):
    features = w_out.shape[0]
    probes = unpack_signs(signs)
    gathered = lax.all_gather(hidden, "shard", axis=0, tiled=True)
    stacked = jnp.concatenate([w_out, probes], axis=0)
    forward = lax.dot_general(
        stacked, gathered, (((1,), (1,)), ((), ())), preferred_element_type=jnp.float32
    )
    output = forward[:features]
    tangent = forward[features:]
    misfit = resid.astype(jnp.float32) + output - target.astype(jnp.float32)
    spread = 1.0 + misfit * misfit
    rooted = jnp.sqrt(spread)
    slopes = (misfit / rooted).astype(jnp.bfloat16)
    bends = (tangent / (spread * rooted)).astype(jnp.bfloat16)
    joined = jnp.concatenate([slopes, bends], axis=0)
    products = jnp.dot(joined, gathered, preferred_element_type=jnp.float32)
    grad_flat = products[:features].reshape(-1, 128)
    curve_flat = products[features:].reshape(-1, 128)
    replicas = lax.axis_size("dp")
    rows_each = grad_flat.shape[0] // replicas
    row_start = lax.axis_index("dp") * rows_each
    grad_mine, curve_mine = (
        lax.psum_scatter(grad_flat, "dp", scatter_dimension=0, tiled=True),
        lax.psum_scatter(curve_flat, "dp", scatter_dimension=0, tiled=True),
    )
    tokens_all = hidden.shape[0] * replicas * lax.axis_size("shard")
    scaling = 1.0 / math.sqrt(tokens_all)
    gradient = grad_mine * scaling
    curvature = curve_mine * scaling
    my_probes = lax.dynamic_slice_in_dim(probes.reshape(-1, 128), row_start, rows_each, 0)
    diag_est = my_probes.astype(jnp.float32) * curvature
    new_m = beta_one * m_old + (1.0 - beta_one) * gradient
    new_v = beta_two * v_old + (1.0 - beta_two) * diag_est * diag_est
    first_fix = 1.0 - beta_one**OPT_STEP
    second_fix = 1.0 - beta_two**OPT_STEP
    update = new_m / first_fix / (jnp.sqrt(new_v / second_fix) + epsilon)
    own_rows = lax.dynamic_slice_in_dim(w_out.reshape(-1, 128), row_start, rows_each, 0)
    fresh_rows = (own_rows.astype(jnp.float32) - learn_rate * update).astype(jnp.bfloat16)
    new_w = lax.all_gather(fresh_rows, "dp", axis=0, tiled=True).reshape(w_out.shape)
    return (new_w, new_m, new_v)


MESH = pl.DeviceIdType.MESH
CHUNK = 512


def plan_of(orders, chunk_mib):
    bits = len(orders[0])
    core_time = 0.0
    free = {}
    ready = {chunk: (0.0, 0) for chunk in range(len(orders))}
    plan = []
    while ready:
        chunk = min(ready, key=lambda c: (max(ready[c][0], core_time) if ready[c][1] else core_time, -ready[c][1], c))
        arrives, step = ready.pop(chunk)
        plan.append((chunk, step))
        core_time = max(core_time, arrives) + (1.2 if step == 0 else 0.4)
        if step == 2 * bits:
            continue
        stage = step if step < bits else 2 * bits - 1 - step
        bit = orders[chunk][stage]
        link = min(bit, 2)
        size = chunk_mib / 2 ** (stage + 1) * (1.0 if step < bits else 0.5)
        if bit == 0:
            cost = size * (2.0 if step < bits else 1.0) * 1.6
        else:
            cost = size * 2 * 11.3
        begin = max(core_time, free.get(link, 0.0))
        free[link] = begin + cost
        ready[chunk] = (begin + cost + 2.5, step + 1)
    return plan


def block_of(mine, done, open_bits, spot):
    index = sum(mine[bit] * 2**bit for bit in done)
    for place, bit in enumerate(open_bits):
        index = index + (spot // 2**place) % 2 * 2**bit
    return index


def kernel(
    orders, plan, cuts, scaling,
    hidden, resid, target, w_out, signs, m_old, v_old,
    w_asm, m_out, v_out,
    hid, res, tar, wts, sig, m_in, v_in,
    stacked, joined, acc, prod, got0, sends, gots, packs,
    load_sem, hid_send, hid_recv, rs_send, rs_recv, ag_send, ag_recv,
):
    shards, tokens, width = hid.shape
    blocks, tall, _ = stacked.shape
    per = tall // 2
    features = blocks * per
    bits = len(orders[0])
    chunks = len(orders)
    me = lax.axis_index("dp")
    my_shard = lax.axis_index("shard")
    mine = [me // 2**bit % 2 for bit in range(bits)]
    partner = [me + (1 - 2 * mine[bit]) * 2**bit for bit in range(bits)]

    own_load = pltpu.make_async_copy(hidden, hid.at[my_shard], load_sem.at[0])
    loads = [
        pltpu.make_async_copy(w_out, wts, load_sem.at[1]),
        pltpu.make_async_copy(signs, sig, load_sem.at[2]),
        pltpu.make_async_copy(m_old, m_in, load_sem.at[3]),
        pltpu.make_async_copy(v_old, v_in, load_sem.at[4]),
    ]
    for part in range(shards):
        columns = pl.ds(part * tokens, tokens)
        loads.append(pltpu.make_async_copy(resid.at[:, columns], res.at[part], load_sem.at[5 + 2 * part]))
        loads.append(pltpu.make_async_copy(target.at[:, columns], tar.at[part], load_sem.at[6 + 2 * part]))
    own_load.start()
    for load in loads:
        load.start()

    barrier = pltpu.get_barrier_semaphore()
    for bit in range(bits):
        pl.semaphore_signal(barrier, inc=1, device_id={"dp": partner[bit]}, device_id_type=MESH)
    for away in range(1, shards):
        other = (my_shard + away) % shards
        pl.semaphore_signal(barrier, inc=1, device_id={"shard": other}, device_id_type=MESH)
    pl.semaphore_wait(barrier, bits + shards - 1)

    hidden_sends = []
    for piece, (start, size) in enumerate(cuts):
        for away in range(1, shards):
            copy = pltpu.make_async_remote_copy(
                src_ref=hidden.at[:, pl.ds(start, size)],
                dst_ref=hid.at[my_shard, :, pl.ds(start, size)],
                send_sem=hid_send.at[away, piece],
                recv_sem=hid_recv.at[away, piece],
                device_id={"shard": (my_shard + away) % shards},
                device_id_type=MESH,
            )
            copy.start()
            hidden_sends.append(copy)

    for load in loads:
        load.wait()

    group = math.lcm(32, per)
    for first in range(0, features, group):

        def spread_signs(column, carry, first=first):
            lanes = pl.ds(pl.multiple_of(column * 128, 128), 128)
            weight = wts[pl.ds(first, group), lanes].astype(jnp.float32)
            shift = lax.broadcasted_iota(jnp.int32, (32, 128), 0)
            words = []
            for word in range(first // 32, (first + group) // 32):
                packed = jnp.broadcast_to(sig[pl.ds(word, 1), lanes], (32, 128))
                words.append((1 - 2 * jnp.bitwise_and(jnp.right_shift(packed, shift), 1)).astype(jnp.float32))
            probe = jnp.concatenate(words, axis=0)
            for part in range(group // per):
                rows = slice(part * per, (part + 1) * per)
                both = jnp.concatenate([weight[rows], probe[rows]], axis=0)
                stacked[first // per + part, :, lanes] = both.astype(jnp.bfloat16)
            return carry

        lax.fori_loop(0, width // 128, spread_signs, 0)

    own_load.wait()
    tile = 4
    last_dims = (((1,), (1,)), ((), ()))

    def forward(part, pieces):
        def one_tile(t, carry):
            rows = pl.ds(pl.multiple_of(t * tile, tile), tile)
            total = None
            for start, size in pieces:
                term = lax.dot_general(
                    stacked[rows, :, pl.ds(start, size)].reshape(tile * tall, size),
                    hid[part, :, pl.ds(start, size)],
                    last_dims,
                    preferred_element_type=jnp.float32,
                )
                total = term if total is None else total + term
            total = total.reshape(tile, tall, tokens)
            if pieces[0][0] > 0:
                total = total + acc[rows]
            if pieces[-1][0] + pieces[-1][1] < width:
                acc[rows] = total
                return carry
            flat = pl.ds(pl.multiple_of(t * tile * per, tile * per), tile * per)
            apart = res[part, flat].astype(jnp.float32) - tar[part, flat].astype(jnp.float32)
            misfit = total[:, :per] + apart.reshape(tile, per, tokens)
            tangent = total[:, per:]
            inverse = lax.rsqrt(1.0 + misfit * misfit)
            slopes = misfit * inverse
            bends = tangent * (inverse * inverse * inverse)
            joined[part, rows] = jnp.concatenate([slopes, bends], axis=1).astype(jnp.bfloat16)
            return carry

        lax.fori_loop(0, blocks // tile, one_tile, 0)

    forward(my_shard, [(0, width)])
    for piece, cut in enumerate(cuts):
        for away in range(1, shards):
            source = (my_shard + shards - away) % shards
            pltpu.make_async_remote_copy(
                src_ref=hidden.at[:, pl.ds(*cut)],
                dst_ref=hid.at[source, :, pl.ds(*cut)],
                send_sem=hid_send.at[away, piece],
                recv_sem=hid_recv.at[away, piece],
                device_id={"shard": source},
                device_id_type=MESH,
            ).wait_recv()
            forward(source, [cut])

    def exchange(chunk, step):
        stage = step if step < bits else 2 * bits - 1 - step
        bit = orders[chunk][stage]
        if step == 0:
            source, landing = prod.at[chunk, :, 1 - mine[0]], got0.at[chunk]
        elif step < bits:
            source, landing = sends[stage - 1].at[chunk], gots[stage - 1].at[chunk]
        else:
            done = set(orders[chunk][: stage + 1])
            where = tuple(mine[b] if b in done else slice(None) for b in reversed(range(bits)))
            source = landing = packs.at[(chunk, *where)]
        send, recv = (rs_send, rs_recv) if step < bits else (ag_send, ag_recv)
        return pltpu.make_async_remote_copy(
            src_ref=source,
            dst_ref=landing,
            send_sem=send.at[stage, chunk],
            recv_sem=recv.at[stage, chunk],
            device_id={"dp": partner[bit]},
            device_id_type=MESH,
        )

    def arrived(chunk, step):
        if step < bits:
            exchange(chunk, step).wait_recv()
            return
        stage = 2 * bits - 1 - step
        bit = orders[chunk][stage]
        done = set(orders[chunk][: stage + 1])
        where = tuple(
            (1 - mine[b] if b == bit else mine[b]) if b in done else slice(None) for b in reversed(range(bits))
        )
        pltpu.make_async_remote_copy(
            src_ref=packs.at[(chunk, *where)],
            dst_ref=packs.at[(chunk, *where)],
            send_sem=ag_send.at[stage, chunk],
            recv_sem=ag_recv.at[stage, chunk],
            device_id={"dp": partner[bit]},
            device_id_type=MESH,
        ).wait_recv()

    def backward(chunk):
        columns = pl.ds(chunk * CHUNK, CHUNK)

        def one_tile(t, carry):
            rows = pl.ds(pl.multiple_of(t * tile, tile), tile)
            total = None
            for part in range(shards):
                term = jnp.dot(
                    joined[part, rows].reshape(tile * tall, tokens),
                    hid[part, :, columns],
                    preferred_element_type=jnp.float32,
                )
                total = term if total is None else total + term
            halves = pl.ds(pl.multiple_of(t * (tile // 2), tile // 2), tile // 2)
            prod[chunk, halves] = total.reshape(tile // 2, 2, tall, CHUNK)
            return carry

        lax.fori_loop(0, blocks // tile, one_tile, 0)

    def received(chunk, stage, spot):
        if stage == 0:
            return got0[chunk, spot]
        return gots[stage - 1][chunk, spot].astype(jnp.float32)

    def fold(chunk, stage):
        order = orders[chunk]
        bit = order[stage]
        before = [b for b in range(bits) if b not in order[:stage]]
        after = [b for b in before if b != bit]
        place = before.index(bit)

        def one_block(spot, carry):
            low = spot % 2**place
            base = low + (spot - low) * 2
            for value, leaves in ((1 - mine[bit], True), (mine[bit], False)):
                full = base + value * 2**place
                index = block_of(mine, order[:stage], before, full)
                total = prod[chunk, index // 2, mine[0]] + received(chunk, stage - 1, full)
                if leaves:
                    sends[stage - 1][chunk, spot] = total.astype(jnp.bfloat16)
                else:
                    prod[chunk, index // 2, mine[0]] = total
            return carry

        lax.fori_loop(0, 2 ** len(after), one_block, 0)

    def step_rows(chunk):
        first_fix = 1.0 - beta_one**OPT_STEP
        second_fix = 1.0 - beta_two**OPT_STEP
        here = tuple(reversed(mine))
        fresh = []
        for part in range(CHUNK // 128):
            lanes = pl.ds(part * 128, 128)
            summed = prod[chunk, me // 2, mine[0], :, lanes]
            landed = gots[bits - 2][chunk, 0, :, lanes].astype(jnp.float32)
            total = (summed + landed) * scaling
            rows = pl.ds(chunk * (CHUNK // 128) + part, per, stride=width // 128)
            first = beta_one * m_in[rows, :] + (1.0 - beta_one) * total[:per]
            second = beta_two * v_in[rows, :] + (1.0 - beta_two) * total[per:] * total[per:]
            m_out[rows, :] = first
            v_out[rows, :] = second
            update = first / first_fix / (jnp.sqrt(second / second_fix) + epsilon)
            weight = stacked[me, :, pl.ds(chunk * CHUNK + part * 128, 128)].astype(jnp.float32)[:per]
            fresh.append(weight - learn_rate * update)
        half = len(fresh) // 2
        for part in range(half):
            both = jnp.concatenate([fresh[part], fresh[half + part]], axis=0)
            packs[(chunk, *here, slice(None), pl.ds(part * 128, 128))] = both.astype(jnp.bfloat16)

    def lay_out(chunk):
        half = CHUNK // 2
        for pair in range(blocks // 2):
            spot = tuple(pair // 2**b % 2 for b in reversed(range(bits - 1)))
            even = packs[(chunk, *spot, 0)].astype(jnp.float32)
            odd = packs[(chunk, *spot, 1)].astype(jnp.float32)
            rows = pl.ds(pair * tall, tall)
            for side in range(2):
                part = slice(side * per, (side + 1) * per)
                both = jnp.concatenate([even[part], odd[part]], axis=0)
                w_asm[rows, pl.ds(chunk * CHUNK + side * half, half)] = both.astype(jnp.bfloat16)

    for chunk, step in plan:
        if step == 0:
            backward(chunk)
        else:
            arrived(chunk, step - 1)
            if step < bits:
                fold(chunk, step)
            elif step == bits:
                step_rows(chunk)
            elif step == 2 * bits:
                lay_out(chunk)
        if step < 2 * bits:
            exchange(chunk, step).start()

    for copy in hidden_sends:
        copy.wait_send()
    for chunk, step in plan:
        if step < 2 * bits:
            exchange(chunk, step).wait_send()


def copy_out(*refs):
    sources, results, sems = refs[:3], refs[3:6], refs[6]
    copies = [pltpu.make_async_copy(a, b, sems.at[i]) for i, (a, b) in enumerate(zip(sources, results))]
    for copy in copies:
        copy.start()
    for copy in copies:
        copy.wait()


def write_out(results):
    return pl.pallas_call(
        copy_out,
        out_shape=tuple(jax.ShapeDtypeStruct(r.shape, r.dtype) for r in results),
        in_specs=[pl.BlockSpec(memory_space=pl.ANY)] * 3,
        out_specs=(pl.BlockSpec(memory_space=pl.ANY),) * 3,
        scratch_shapes=[pltpu.SemaphoreType.DMA((3,))],
        compiler_params=pltpu.CompilerParams(vmem_limit_bytes=1024 * 1024, has_side_effects=True),
    )(*results)


def in_one_kernel(hidden, resid, target, w_out, signs, m_old, v_old):
    blocks, shards = lax.axis_size("dp"), lax.axis_size("shard")
    features, width = w_out.shape
    tokens = hidden.shape[0]
    per = features // blocks
    tall = 2 * per
    bits = blocks.bit_length() - 1
    chunks = width // CHUNK
    orders = [list(range(bits)) for _ in range(chunks)]
    if bits > 2:
        orders[0][1:3] = [2, 1]
    plan = plan_of(orders, features * 2 * CHUNK * 2 / 2**20)
    cuts = [(0, width - CHUNK), (width - CHUNK, CHUNK)]
    scaling = 1.0 / math.sqrt(tokens * blocks * shards)
    bf16, f32 = jnp.bfloat16, jnp.float32
    levels = [pltpu.VMEM((chunks, blocks >> (stage + 1), tall, CHUNK), bf16) for stage in range(1, bits)]
    dma = pltpu.SemaphoreType.DMA
    anywhere = pl.BlockSpec(memory_space=pl.ANY)
    results = pl.pallas_call(
        functools.partial(kernel, orders, plan, cuts, scaling),
        out_shape=(
            pltpu.VMEM(w_out.shape, bf16),
            pltpu.VMEM(m_old.shape, f32),
            pltpu.VMEM(v_old.shape, f32),
        ),
        in_specs=[anywhere] * 7,
        out_specs=(pl.BlockSpec(memory_space=pltpu.VMEM),) * 3,
        scratch_shapes=[
            pltpu.VMEM((shards, tokens, width), bf16),
            pltpu.VMEM((shards, features, tokens), bf16),
            pltpu.VMEM((shards, features, tokens), bf16),
            pltpu.VMEM(w_out.shape, bf16),
            pltpu.VMEM(signs.shape, jnp.int32),
            pltpu.VMEM(m_old.shape, f32),
            pltpu.VMEM(v_old.shape, f32),
            pltpu.VMEM((blocks, tall, width), bf16),
            pltpu.VMEM((shards, blocks, tall, tokens), bf16),
            pltpu.VMEM((blocks, tall, tokens), f32),
            pltpu.VMEM((chunks, blocks // 2, 2, tall, CHUNK), f32),
            pltpu.VMEM((chunks, blocks // 2, tall, CHUNK), f32),
            levels,
            levels,
            pltpu.VMEM((chunks, *((2,) * bits), tall, CHUNK // 2), bf16),
            dma((5 + 2 * shards,)),
            dma((shards, len(cuts))),
            dma((shards, len(cuts))),
            dma((bits, chunks)),
            dma((bits, chunks)),
            dma((bits, chunks)),
            dma((bits, chunks)),
        ],
        compiler_params=pltpu.CompilerParams(
            collective_id=0, has_side_effects=True, vmem_limit_bytes=54 * 1024 * 1024
        ),
    )(hidden, resid, target, w_out, signs, m_old, v_old)
    return write_out(results)


def fits(hidden, w_out):
    blocks, shards = lax.axis_size("dp"), lax.axis_size("shard")
    features, width = w_out.shape
    per = features // blocks
    return (
        shards > 1
        and blocks >= 4
        and blocks & (blocks - 1) == 0
        and features % (blocks * 8) == 0
        and features % math.lcm(32, per) == 0
        and width % CHUNK == 0
        and width > CHUNK
        and hidden.shape[0] % 128 == 0
    )


def either(hidden, resid, target, w_out, signs, m_old, v_old):
    run = in_one_kernel if fits(hidden, w_out) else on_device
    return run(hidden, resid, target, w_out, signs, m_old, v_old)


def solution(mesh):
    return jax.shard_map(
        either,
        mesh=mesh,
        in_specs=(
            P(("dp", "shard"), None),
            P("shard", "dp"),
            P("shard", "dp"),
            P("shard", None),
            P("shard", None),
            P(("shard", "dp"), None),
            P(("shard", "dp"), None),
        ),
        out_specs=(P("shard", None), P(("shard", "dp"), None), P(("shard", "dp"), None)),
        check_vma=False,
    )
```

```python
import functools
import math
import random

import jax
import jax.numpy as jnp
from jax import lax
from jax.experimental import pallas as pl
from jax.experimental.pallas import tpu as pltpu
from jax.sharding import PartitionSpec as P

OPT_STEP = 10


beta_one = 0.9
beta_two = 0.999
learn_rate = 0.15
epsilon = 0.0001


def unpack_signs(signs):
    shifts = jnp.arange(32, dtype=jnp.int32)
    bit_values = jnp.bitwise_and(jnp.right_shift(signs[:, None, :], shifts[None, :, None]), 1)
    return (1 - 2 * bit_values).reshape(signs.shape[0] * 32, signs.shape[1]).astype(jnp.bfloat16)


def on_device(hidden, resid, target, w_out, signs, m_old, v_old):
    features = w_out.shape[0]
    probes = unpack_signs(signs)
    gathered = lax.all_gather(hidden, "shard", axis=0, tiled=True)
    stacked = jnp.concatenate([w_out, probes], axis=0)
    forward = lax.dot_general(
        stacked, gathered, (((1,), (1,)), ((), ())), preferred_element_type=jnp.float32
    )
    output = forward[:features]
    tangent = forward[features:]
    misfit = resid.astype(jnp.float32) + output - target.astype(jnp.float32)
    spread = 1.0 + misfit * misfit
    rooted = jnp.sqrt(spread)
    slopes = (misfit / rooted).astype(jnp.bfloat16)
    bends = (tangent / (spread * rooted)).astype(jnp.bfloat16)
    joined = jnp.concatenate([slopes, bends], axis=0)
    products = jnp.dot(joined, gathered, preferred_element_type=jnp.float32)
    grad_flat = products[:features].reshape(-1, 128)
    curve_flat = products[features:].reshape(-1, 128)
    replicas = lax.axis_size("dp")
    rows_each = grad_flat.shape[0] // replicas
    row_start = lax.axis_index("dp") * rows_each
    grad_mine, curve_mine = (
        lax.psum_scatter(grad_flat, "dp", scatter_dimension=0, tiled=True),
        lax.psum_scatter(curve_flat, "dp", scatter_dimension=0, tiled=True),
    )
    tokens_all = hidden.shape[0] * replicas * lax.axis_size("shard")
    scaling = 1.0 / math.sqrt(tokens_all)
    gradient = grad_mine * scaling
    curvature = curve_mine * scaling
    my_probes = lax.dynamic_slice_in_dim(probes.reshape(-1, 128), row_start, rows_each, 0)
    diag_est = my_probes.astype(jnp.float32) * curvature
    new_m = beta_one * m_old + (1.0 - beta_one) * gradient
    new_v = beta_two * v_old + (1.0 - beta_two) * diag_est * diag_est
    first_fix = 1.0 - beta_one**OPT_STEP
    second_fix = 1.0 - beta_two**OPT_STEP
    update = new_m / first_fix / (jnp.sqrt(new_v / second_fix) + epsilon)
    own_rows = lax.dynamic_slice_in_dim(w_out.reshape(-1, 128), row_start, rows_each, 0)
    fresh_rows = (own_rows.astype(jnp.float32) - learn_rate * update).astype(jnp.bfloat16)
    new_w = lax.all_gather(fresh_rows, "dp", axis=0, tiled=True).reshape(w_out.shape)
    return (new_w, new_m, new_v)


MESH = pl.DeviceIdType.MESH
CHUNK = 256


def simulate(orders, chunk_mib, rank, weights, spread):
    bits = len(orders[0])
    core_time = 0.0
    free = {}
    ready = {chunk: (0.0, 1) for chunk in range(len(orders))}
    plan = []
    while ready:
        due = [chunk for chunk in ready if ready[chunk][0] <= core_time]
        if due:
            chunk = min(due, key=lambda c: (weights[ready[c][1]] + spread * rank[c], c))
        else:
            chunk = min(ready, key=lambda c: (ready[c][0], c))
        arrives, step = ready.pop(chunk)
        plan.append((chunk, step))
        core_time = max(core_time, arrives) + (0.8 if step == 1 else 0.25 if step == bits else 0.12)
        if step == 2 * bits:
            continue
        stage = step if step < bits else 2 * bits - 1 - step
        bit = orders[chunk][stage]
        size = chunk_mib / 2 ** (stage + 1) * (2.0 if step < bits else 1.0)
        if bit == 0:
            links, pace, flight = {"core": 1.0}, 1.6, 1.1
        elif bit == 1:
            links, pace, flight = {"y": 1.0}, 22.6, 2.4
        elif bit == 2:
            links, pace, flight = {"z": 1.0}, 22.6, 2.4
        else:
            links, pace, flight = {"z": 1.0, "mid": 2.0}, 22.6, 3.2
        begin = max([core_time] + [free.get(link, 0.0) for link in links])
        for link, share in links.items():
            free[link] = begin + size * pace * share
        ready[chunk] = (max(free[link] for link in links) + flight, step + 1)
    return core_time, plan


def plan_of(orders, chunk_mib):
    draw = random.Random(0)
    bits, chunks = len(orders[0]), len(orders)
    best = None
    for _ in range(600):
        rank = list(range(chunks))
        draw.shuffle(rank)
        weights = [draw.choice([0, 5, 20, 100]) * draw.random() for _ in range(2 * bits + 1)]
        found = simulate(orders, chunk_mib, rank, weights, draw.choice([0, 1, 3]))
        if best is None or found[0] < best[0]:
            best = found
    return best[1]


def kernel(
    orders, plan, cuts, scaling,
    hidden, resid, target, w_out, signs, m_old, v_old,
    w_asm, m_out, v_out,
    hid, res, tar, wts, sig, m_in, v_in,
    stacked, apart, joined, acc, prod, sends, gots, packs,
    load_sem, pair_send, pair_recv, hid_send, hid_recv, fwd_send, fwd_recv, rs_send, rs_recv, ag_send, ag_recv,
):
    width = hid.shape[1]
    tokens = hidden.shape[0]
    shards = hid.shape[0] // tokens // 2
    chips, tall, _ = stacked.shape
    per = tall // 2
    features = chips * tall
    bits = len(orders[0])
    me = lax.axis_index("dp")
    my_shard = lax.axis_index("shard")
    mine = [me // 2**bit % 2 for bit in range(bits)]
    partner = [me + (1 - 2 * mine[bit]) * 2**bit for bit in range(bits)]
    core = mine[0]

    def span(shard, side):
        return pl.ds(pl.multiple_of((shard * 2 + side) * tokens, tokens), tokens)

    own_load = pltpu.make_async_copy(hidden, hid.at[span(my_shard, core)], load_sem.at[0])
    loads = [
        pltpu.make_async_copy(w_out, wts, load_sem.at[1]),
        pltpu.make_async_copy(signs, sig, load_sem.at[2]),
        pltpu.make_async_copy(m_old, m_in, load_sem.at[3]),
        pltpu.make_async_copy(v_old, v_in, load_sem.at[4]),
        pltpu.make_async_copy(resid, res.at[core], load_sem.at[5]),
        pltpu.make_async_copy(target, tar.at[core], load_sem.at[6]),
    ]
    for load in loads[:2]:
        load.start()
    own_load.start()

    barrier = pltpu.get_barrier_semaphore()
    for bit in range(bits):
        pl.semaphore_signal(barrier, inc=1, device_id={"dp": partner[bit]}, device_id_type=MESH)
    for away in range(1, shards):
        other = (my_shard + away) % shards
        pl.semaphore_signal(barrier, inc=1, device_id={"shard": other}, device_id_type=MESH)
    pl.semaphore_wait(barrier, bits + shards - 1)

    hidden_sends = []
    for piece, (start, size) in enumerate(cuts):
        for away in range(1, shards):
            copy = pltpu.make_async_remote_copy(
                src_ref=hidden.at[:, pl.ds(start, size)],
                dst_ref=hid.at[span(my_shard, core), pl.ds(start, size)],
                send_sem=hid_send.at[away, piece],
                recv_sem=hid_recv.at[away, piece],
                device_id={"shard": (my_shard + away) % shards},
                device_id_type=MESH,
            )
            copy.start()
            hidden_sends.append(copy)

    def to_pair(source, landing, index):
        return pltpu.make_async_remote_copy(
            src_ref=source,
            dst_ref=landing,
            send_sem=pair_send.at[index],
            recv_sem=pair_recv.at[index],
            device_id={"dp": partner[0]},
            device_id_type=MESH,
        )

    pair_sends = [
        to_pair(hidden, hid.at[span(my_shard, core)], 0),
        to_pair(resid, res.at[core], 1),
        to_pair(target, tar.at[core], 2),
    ]
    for copy in pair_sends:
        copy.start()
    for load in loads[2:]:
        load.start()

    def pair_arrives(source, landing, index):
        to_pair(source, landing, index).wait_recv()

    loads[0].wait()
    loads[1].wait()
    group = math.lcm(32, tall)
    for first in range(0, features, group):

        def spread_signs(column, carry, first=first):
            lanes = pl.ds(pl.multiple_of(column * 128, 128), 128)
            weight = wts[pl.ds(first, group), lanes].astype(jnp.float32)
            shift = lax.broadcasted_iota(jnp.int32, (32, 128), 0)
            words = []
            for word in range(first // 32, (first + group) // 32):
                packed = jnp.broadcast_to(sig[pl.ds(word, 1), lanes], (32, 128))
                words.append((1 - 2 * jnp.bitwise_and(jnp.right_shift(packed, shift), 1)).astype(jnp.float32))
            probe = jnp.concatenate(words, axis=0)
            for part in range(group // tall):
                low = slice(part * tall, part * tall + per)
                high = slice(part * tall + per, (part + 1) * tall)
                both = [jnp.where(core == 0, matrix[low], matrix[high]) for matrix in (weight, probe)]
                stacked[first // tall + part, :, lanes] = jnp.concatenate(both, axis=0).astype(jnp.bfloat16)
            return carry

        lax.fori_loop(0, width // 128, spread_signs, 0)

    own_load.wait()
    tile = chips // 2
    last_dims = (((1,), (1,)), ((), ()))

    def differ(side):
        def one_chip(chip, carry):
            rows = pl.ds(pl.multiple_of(chip * tall, tall), tall)
            gap = res[side, rows].astype(jnp.float32) - tar[side, rows].astype(jnp.float32)
            apart[side, chip] = jnp.where(core == 0, gap[:per], gap[per:])
            return carry

        lax.fori_loop(0, chips, one_chip, 0)

    def forward(shard, side, pieces, slot):
        token_rows = span(shard, side)
        columns_of = pl.ds(pl.multiple_of(shard * tokens, tokens), tokens)

        def one_tile(t, carry):
            rows = pl.ds(pl.multiple_of(t * tile, tile), tile)
            total = None
            for start, size in pieces:
                term = lax.dot_general(
                    stacked[rows, :, pl.ds(start, size)].reshape(tile * tall, size),
                    hid[token_rows, pl.ds(start, size)],
                    last_dims,
                    preferred_element_type=jnp.float32,
                )
                total = term if total is None else total + term
            total = total.reshape(tile, tall, tokens)
            if pieces[0][0] > 0:
                total = total + acc[slot, rows]
            if pieces[-1][0] + pieces[-1][1] < width:
                acc[slot, rows] = total
                return carry
            misfit = total[:, :per] + apart[side, rows, :, columns_of]
            tangent = total[:, per:]
            inverse = lax.rsqrt(1.0 + misfit * misfit)
            slopes = misfit * inverse
            bends = tangent * (inverse * inverse * inverse)
            joined[rows, :, token_rows] = jnp.concatenate([slopes, bends], axis=1).astype(jnp.bfloat16)
            return carry

        lax.fori_loop(0, chips // tile, one_tile, 0)

    loads[4].wait()
    loads[5].wait()
    differ(core)
    with jax.named_scope("own"):
        forward(my_shard, core, [(0, width)], 0)
    pair_arrives(resid, res.at[1 - core], 1)
    pair_arrives(target, tar.at[1 - core], 2)
    differ(1 - core)
    pair_arrives(hidden, hid.at[span(my_shard, 1 - core)], 0)
    with jax.named_scope("pair"):
        forward(my_shard, 1 - core, [(0, width)], 0)
    loads[2].wait()
    loads[3].wait()

    def relay(shard, side, away, piece):
        where = hid.at[span(shard, side), pl.ds(*cuts[piece])]
        return pltpu.make_async_remote_copy(
            src_ref=where,
            dst_ref=where,
            send_sem=fwd_send.at[away, piece],
            recv_sem=fwd_recv.at[away, piece],
            device_id={"dp": partner[0]},
            device_id_type=MESH,
        )

    relays = []
    for piece, cut in enumerate(cuts):
        for away in range(1, shards):
            source = (my_shard + shards - away) % shards
            arriving = pltpu.make_async_remote_copy(
                src_ref=hidden.at[:, pl.ds(*cut)],
                dst_ref=hid.at[span(source, core), pl.ds(*cut)],
                send_sem=hid_send.at[away, piece],
                recv_sem=hid_recv.at[away, piece],
                device_id={"shard": source},
                device_id_type=MESH,
            )
            with jax.named_scope(f"x{piece}"):
                arriving.wait_recv()
            copy = relay(source, core, away, piece)
            copy.start()
            relays.append(copy)
            with jax.named_scope(f"f{piece}"):
                forward(source, core, [cut], (away - 1) * 2)
            with jax.named_scope(f"r{piece}"):
                relay(source, 1 - core, away, piece).wait_recv()
            with jax.named_scope(f"g{piece}"):
                forward(source, 1 - core, [cut], (away - 1) * 2 + 1)

    def exchange(chunk, step):
        stage = step if step < bits else 2 * bits - 1 - step
        bit = orders[chunk][stage]
        if step < bits:
            source, landing = sends[stage - 1].at[chunk], gots[stage - 1].at[chunk]
        else:
            done = set(orders[chunk][: stage + 1])
            where = tuple(mine[b] if b in done else slice(None) for b in reversed(range(bits)))
            source = landing = packs.at[(chunk, *where)]
        send, recv = (rs_send, rs_recv) if step < bits else (ag_send, ag_recv)
        return pltpu.make_async_remote_copy(
            src_ref=source,
            dst_ref=landing,
            send_sem=send.at[stage, chunk],
            recv_sem=recv.at[stage, chunk],
            device_id={"dp": partner[bit]},
            device_id_type=MESH,
        )

    def arrived(chunk, step):
        if step < bits:
            exchange(chunk, step).wait_recv()
            return
        stage = 2 * bits - 1 - step
        bit = orders[chunk][stage]
        done = set(orders[chunk][: stage + 1])
        where = tuple(
            (1 - mine[b] if b == bit else mine[b]) if b in done else slice(None) for b in reversed(range(bits))
        )
        pltpu.make_async_remote_copy(
            src_ref=packs.at[(chunk, *where)],
            dst_ref=packs.at[(chunk, *where)],
            send_sem=ag_send.at[stage, chunk],
            recv_sem=ag_recv.at[stage, chunk],
            device_id={"dp": partner[bit]},
            device_id_type=MESH,
        ).wait_recv()

    def backward(chunk):
        columns = pl.ds(chunk * CHUNK, CHUNK)
        place = orders[chunk][1] - 1
        for value, leaves in ((1 - mine[place + 1], True), (mine[place + 1], False)):
            if place == 0:
                rows = joined.reshape(chips // 2, 2, tall, joined.shape[2])[:, value]
            else:
                outer = chips // 2 ** (place + 1)
                rows = joined.reshape(outer, 2, 2**place, tall, joined.shape[2])[:, value]
            total = jnp.dot(
                rows.reshape(chips // 2 * tall, joined.shape[2]),
                hid[:, columns],
                preferred_element_type=jnp.float32,
            ).reshape(chips // 2, tall, CHUNK)
            if leaves:
                sends[0][chunk] = total.astype(jnp.bfloat16)
                exchange(chunk, 1).start()
            else:
                prod[chunk] = total

    def spot_of(chunk, stage):
        order = orders[chunk]
        open_bits = [b for b in range(1, bits) if b != order[1]]
        return [b for b in open_bits if b not in order[2:stage]], open_bits

    def fold(chunk, stage):
        order = orders[chunk]
        bit = order[stage]
        before, open_bits = spot_of(chunk, stage)
        after = [b for b in before if b != bit]
        for value, leaves in ((1 - mine[bit], True), (mine[bit], False)):
            for spot in range(2 ** len(after)):
                values = {b: spot // 2**i % 2 for i, b in enumerate(after)}
                values[bit] = value
                full = sum(values[b] * 2**i for i, b in enumerate(before))
                for b in order[2:stage]:
                    values[b] = mine[b]
                index = sum(values[b] * 2**i for i, b in enumerate(open_bits))
                total = prod[chunk, index] + gots[stage - 2][chunk, full].astype(jnp.float32)
                if leaves:
                    sends[stage - 1][chunk, spot] = total.astype(jnp.bfloat16)
                else:
                    prod[chunk, index] = total
            if leaves:
                exchange(chunk, stage).start()

    def step_rows(chunk):
        first_fix = 1.0 - beta_one**OPT_STEP
        second_fix = 1.0 - beta_two**OPT_STEP
        here = tuple(reversed(mine))
        _, open_bits = spot_of(chunk, 2)
        index = sum(mine[b] * 2**i for i, b in enumerate(open_bits))
        fresh = []
        for part in range(CHUNK // 128):
            lanes = pl.ds(part * 128, 128)
            summed = prod[chunk, index, :, lanes]
            landed = gots[bits - 2][chunk, 0, :, lanes].astype(jnp.float32)
            total = (summed + landed) * scaling
            rows = pl.ds(chunk * (CHUNK // 128) + part, per, stride=width // 128)
            first = beta_one * m_in[rows, :] + (1.0 - beta_one) * total[:per]
            second = beta_two * v_in[rows, :] + (1.0 - beta_two) * total[per:] * total[per:]
            m_out[rows, :] = first
            v_out[rows, :] = second
            update = first / first_fix / (jnp.sqrt(second / second_fix) + epsilon)
            weight = stacked[me // 2, :, pl.ds(chunk * CHUNK + part * 128, 128)].astype(jnp.float32)[:per]
            fresh.append(weight - learn_rate * update)
        half = len(fresh) // 2
        for part in range(half):
            both = jnp.concatenate([fresh[part], fresh[half + part]], axis=0)
            packs[(chunk, *here, slice(None), pl.ds(part * 128, 128))] = both.astype(jnp.bfloat16)

    def lay_out(chunk):
        half = CHUNK // 2
        for pair in range(chips):
            spot = tuple(pair // 2**b % 2 for b in reversed(range(bits - 1)))
            even = packs[(chunk, *spot, 0)].astype(jnp.float32)
            odd = packs[(chunk, *spot, 1)].astype(jnp.float32)
            rows = pl.ds(pair * tall, tall)
            for side in range(2):
                part = slice(side * per, (side + 1) * per)
                both = jnp.concatenate([even[part], odd[part]], axis=0)
                w_asm[rows, pl.ds(chunk * CHUNK + side * half, half)] = both.astype(jnp.bfloat16)

    for chunk, step in plan:
        if step == 1:
            with jax.named_scope(f"b{chunk}"):
                backward(chunk)
            continue
        with jax.named_scope(f"w{chunk}_{step}"):
            arrived(chunk, step - 1)
        with jax.named_scope(f"k{chunk}_{step}"):
            if step < bits:
                fold(chunk, step)
            elif step == bits:
                step_rows(chunk)
            elif step == 2 * bits:
                lay_out(chunk)
        if bits <= step < 2 * bits:
            exchange(chunk, step).start()

    for copy in hidden_sends + pair_sends + relays:
        copy.wait_send()
    for chunk, step in plan:
        if step < 2 * bits:
            exchange(chunk, step).wait_send()


def copy_out(*refs):
    sources, results, sems = refs[:3], refs[3:6], refs[6]
    copies = [pltpu.make_async_copy(a, b, sems.at[i]) for i, (a, b) in enumerate(zip(sources, results))]
    for copy in copies:
        copy.start()
    for copy in copies:
        copy.wait()


def write_out(results):
    return pl.pallas_call(
        copy_out,
        out_shape=tuple(jax.ShapeDtypeStruct(r.shape, r.dtype) for r in results),
        in_specs=[pl.BlockSpec(memory_space=pl.ANY)] * 3,
        out_specs=(pl.BlockSpec(memory_space=pl.ANY),) * 3,
        scratch_shapes=[pltpu.SemaphoreType.DMA((3,))],
        compiler_params=pltpu.CompilerParams(vmem_limit_bytes=1024 * 1024, has_side_effects=True),
    )(*results)


def in_one_kernel(hidden, resid, target, w_out, signs, m_old, v_old):
    blocks, shards = lax.axis_size("dp"), lax.axis_size("shard")
    features, width = w_out.shape
    tokens = hidden.shape[0]
    per = features // blocks
    tall = 2 * per
    chips = blocks // 2
    bits = blocks.bit_length() - 1
    chunks = width // CHUNK
    orders = [list(range(bits)) for _ in range(chunks)]
    for chunk in range(chunks // 5):
        orders[chunk][1:3] = [2, 1]
    plan = plan_of(orders, features * 2 * CHUNK / 2**20)
    half = width // 2
    cuts = [(0, half), (half, half - 2 * CHUNK), (width - 2 * CHUNK, CHUNK), (width - CHUNK, CHUNK)]
    scaling = 1.0 / math.sqrt(tokens * blocks * shards)
    bf16, f32 = jnp.bfloat16, jnp.float32
    levels = [pltpu.VMEM((chunks, chips >> stage, tall, CHUNK), bf16) for stage in range(1, bits)]
    dma = pltpu.SemaphoreType.DMA
    anywhere = pl.BlockSpec(memory_space=pl.ANY)
    results = pl.pallas_call(
        functools.partial(kernel, orders, plan, cuts, scaling),
        out_shape=(
            pltpu.VMEM(w_out.shape, bf16),
            pltpu.VMEM(m_old.shape, f32),
            pltpu.VMEM(v_old.shape, f32),
        ),
        in_specs=[anywhere] * 7,
        out_specs=(pl.BlockSpec(memory_space=pltpu.VMEM),) * 3,
        scratch_shapes=[
            pltpu.VMEM((shards * 2 * tokens, width), bf16),
            pltpu.VMEM((2, *resid.shape), bf16),
            pltpu.VMEM((2, *target.shape), bf16),
            pltpu.VMEM(w_out.shape, bf16),
            pltpu.VMEM(signs.shape, jnp.int32),
            pltpu.VMEM(m_old.shape, f32),
            pltpu.VMEM(v_old.shape, f32),
            pltpu.VMEM((chips, tall, width), bf16),
            pltpu.VMEM((2, chips, per, shards * tokens), f32),
            pltpu.VMEM((chips, tall, shards * 2 * tokens), bf16),
            pltpu.VMEM((2 * (shards - 1), chips, tall, tokens), f32),
            pltpu.VMEM((chunks, chips // 2, tall, CHUNK), f32),
            levels,
            levels,
            pltpu.VMEM((chunks, *((2,) * bits), tall, CHUNK // 2), bf16),
            dma((7,)),
            dma((3,)),
            dma((3,)),
            dma((shards, len(cuts))),
            dma((shards, len(cuts))),
            dma((shards, len(cuts))),
            dma((shards, len(cuts))),
            dma((bits, chunks)),
            dma((bits, chunks)),
            dma((bits, chunks)),
            dma((bits, chunks)),
        ],
        compiler_params=pltpu.CompilerParams(
            collective_id=0, has_side_effects=True, vmem_limit_bytes=54 * 1024 * 1024
        ),
    )(hidden, resid, target, w_out, signs, m_old, v_old)
    return write_out(results)


def fits(hidden, w_out):
    blocks, shards = lax.axis_size("dp"), lax.axis_size("shard")
    features, width = w_out.shape
    per = features // blocks
    return (
        shards > 1
        and blocks >= 8
        and blocks & (blocks - 1) == 0
        and features % (blocks * 8) == 0
        and features % math.lcm(32, 2 * per) == 0
        and width % CHUNK == 0
        and width >= 8 * CHUNK
        and hidden.shape[0] % 128 == 0
    )


def either(hidden, resid, target, w_out, signs, m_old, v_old):
    run = in_one_kernel if fits(hidden, w_out) else on_device
    return run(hidden, resid, target, w_out, signs, m_old, v_old)


def solution(mesh):
    return jax.shard_map(
        either,
        mesh=mesh,
        in_specs=(
            P(("dp", "shard"), None),
            P("shard", "dp"),
            P("shard", "dp"),
            P("shard", None),
            P("shard", None),
            P(("shard", "dp"), None),
            P(("shard", "dp"), None),
        ),
        out_specs=(P("shard", None), P(("shard", "dp"), None), P(("shard", "dp"), None)),
        check_vma=False,
    )
```

```python
import functools
import math

import jax
import jax.numpy as jnp
from jax import lax
from jax.experimental import pallas as pl
from jax.experimental.pallas import tpu as pltpu
from jax.sharding import PartitionSpec as P

OPT_STEP = 10


beta_one = 0.9
beta_two = 0.999
learn_rate = 0.15
epsilon = 0.0001


def unpack_signs(signs):
    shifts = jnp.arange(32, dtype=jnp.int32)
    bit_values = jnp.bitwise_and(jnp.right_shift(signs[:, None, :], shifts[None, :, None]), 1)
    return (1 - 2 * bit_values).reshape(signs.shape[0] * 32, signs.shape[1]).astype(jnp.bfloat16)


def on_device(hidden, resid, target, w_out, signs, m_old, v_old):
    features = w_out.shape[0]
    probes = unpack_signs(signs)
    gathered = lax.all_gather(hidden, "shard", axis=0, tiled=True)
    stacked = jnp.concatenate([w_out, probes], axis=0)
    forward = lax.dot_general(
        stacked, gathered, (((1,), (1,)), ((), ())), preferred_element_type=jnp.float32
    )
    output = forward[:features]
    tangent = forward[features:]
    misfit = resid.astype(jnp.float32) + output - target.astype(jnp.float32)
    spread = 1.0 + misfit * misfit
    rooted = jnp.sqrt(spread)
    slopes = (misfit / rooted).astype(jnp.bfloat16)
    bends = (tangent / (spread * rooted)).astype(jnp.bfloat16)
    joined = jnp.concatenate([slopes, bends], axis=0)
    products = jnp.dot(joined, gathered, preferred_element_type=jnp.float32)
    grad_flat = products[:features].reshape(-1, 128)
    curve_flat = products[features:].reshape(-1, 128)
    replicas = lax.axis_size("dp")
    rows_each = grad_flat.shape[0] // replicas
    row_start = lax.axis_index("dp") * rows_each
    grad_mine, curve_mine = (
        lax.psum_scatter(grad_flat, "dp", scatter_dimension=0, tiled=True),
        lax.psum_scatter(curve_flat, "dp", scatter_dimension=0, tiled=True),
    )
    tokens_all = hidden.shape[0] * replicas * lax.axis_size("shard")
    scaling = 1.0 / math.sqrt(tokens_all)
    gradient = grad_mine * scaling
    curvature = curve_mine * scaling
    my_probes = lax.dynamic_slice_in_dim(probes.reshape(-1, 128), row_start, rows_each, 0)
    diag_est = my_probes.astype(jnp.float32) * curvature
    new_m = beta_one * m_old + (1.0 - beta_one) * gradient
    new_v = beta_two * v_old + (1.0 - beta_two) * diag_est * diag_est
    first_fix = 1.0 - beta_one**OPT_STEP
    second_fix = 1.0 - beta_two**OPT_STEP
    update = new_m / first_fix / (jnp.sqrt(new_v / second_fix) + epsilon)
    own_rows = lax.dynamic_slice_in_dim(w_out.reshape(-1, 128), row_start, rows_each, 0)
    fresh_rows = (own_rows.astype(jnp.float32) - learn_rate * update).astype(jnp.bfloat16)
    new_w = lax.all_gather(fresh_rows, "dp", axis=0, tiled=True).reshape(w_out.shape)
    return (new_w, new_m, new_v)


MESH = pl.DeviceIdType.MESH
CHUNK = 256


ROUTES = [
    [[1], [2], [3], [-1], [1], [2, 3]],
    [[1], [2], [3], [-1], [3], [2], [1]],
    [[1], [2], [3], [-1], [3], [1], [2]],
    [[2], [1], [3], [-1], [2, 3], [1]],
    [[1], [2, 3], [-1], [3], [1], [2]],
    [[1], [2], [3], [-1], [2, 3], [1]],
    [[2, 3], [1], [-1], [3], [2], [1]],
    [[1], [2, 3], [-1], [3], [2], [1]],
    [[1], [2, 3], [-1], [2, 3], [1]],
    [[1], [2, 3], [-1], [3], [2], [1]],
]
ORDER = [
    7, 6, 8, 3, 1, 9, 2, 7, 4, 0, 5, 8, 6, 1, 3, 7, 9, 8, 2, 1, 7, 4, 9, 8,
    2, 0, 1, 7, 5, 4, 6, 9, 3, 2, 0, 8, 1, 8, 7, 5, 7, 4, 6, 9, 3, 2, 4, 0,
    1, 9, 5, 6, 2, 9, 0, 3, 1, 4, 1, 4, 6, 5, 6, 2, 3, 2, 3, 0, 5, 0, 5,
]


def masks_of(group):
    masks = [0]
    for bit in group:
        masks = masks + [mask | 1 << bit for mask in masks]
    return masks


def routes_of(bits):
    split = [[group for group in route if group] for route in ROUTES]
    return [(route[: route.index([-1])], route[route.index([-1]) + 1 :] + [[0]]) for route in split]


def kernel(
    routes, order, cuts, scaling,
    hidden, resid, target, w_out, signs, m_old, v_old,
    w_asm, m_out, v_out,
    hid, res, tar, wts, sig, m_in, v_in,
    stacked, apart, joined, acc, prod, sends, gots, packs,
    load_sem, pair_send, pair_recv, hid_send, hid_recv, fwd_send, fwd_recv, rs_send, rs_recv, ag_send, ag_recv,
):
    width = hid.shape[1]
    tokens = hidden.shape[0]
    shards = hid.shape[0] // tokens // 2
    chips, tall, _ = stacked.shape
    per = tall // 2
    features = chips * tall
    bits = (2 * chips).bit_length() - 1
    me = lax.axis_index("dp")
    my_shard = lax.axis_index("shard")
    mine = [me // 2**bit % 2 for bit in range(bits)]
    core = mine[0]

    def device_of(mask):
        return {"dp": me + sum((1 - 2 * mine[bit]) * 2**bit for bit in range(bits) if mask >> bit & 1)}

    def span(shard, side):
        return pl.ds(pl.multiple_of((shard * 2 + side) * tokens, tokens), tokens)

    own_load = pltpu.make_async_copy(hidden, hid.at[span(my_shard, core)], load_sem.at[0])
    loads = [
        pltpu.make_async_copy(w_out, wts, load_sem.at[1]),
        pltpu.make_async_copy(signs, sig, load_sem.at[2]),
        pltpu.make_async_copy(m_old, m_in, load_sem.at[3]),
        pltpu.make_async_copy(v_old, v_in, load_sem.at[4]),
        pltpu.make_async_copy(resid, res.at[core], load_sem.at[5]),
        pltpu.make_async_copy(target, tar.at[core], load_sem.at[6]),
    ]
    for load in loads[:2]:
        load.start()
    own_load.start()

    barrier = pltpu.get_barrier_semaphore()
    meets = {mask for route in routes for stages in route for group in stages for mask in masks_of(group)[1:]}
    for mask in sorted(meets):
        pl.semaphore_signal(barrier, inc=1, device_id=device_of(mask), device_id_type=MESH)
    for away in range(1, shards):
        other = (my_shard + away) % shards
        pl.semaphore_signal(barrier, inc=1, device_id={"shard": other}, device_id_type=MESH)
    pl.semaphore_wait(barrier, len(meets) + shards - 1)

    for piece, (start, size) in enumerate(cuts):
        for away in range(1, shards):
            copy = pltpu.make_async_remote_copy(
                src_ref=hidden.at[:, pl.ds(start, size)],
                dst_ref=hid.at[span(my_shard, core), pl.ds(start, size)],
                send_sem=hid_send.at[away - 1],
                recv_sem=hid_recv.at[(away - 1) * len(cuts) + piece],
                device_id={"shard": (my_shard + away) % shards},
                device_id_type=MESH,
            )
            copy.start()

    def to_pair(source, landing, index):
        return pltpu.make_async_remote_copy(
            src_ref=source,
            dst_ref=landing,
            send_sem=pair_send.at[index],
            recv_sem=pair_recv.at[index],
            device_id=device_of(1),
            device_id_type=MESH,
        )

    pair_sends = [
        to_pair(hidden, hid.at[span(my_shard, core)], 0),
        to_pair(resid, res.at[core], 1),
        to_pair(target, tar.at[core], 2),
    ]
    for copy in pair_sends:
        copy.start()
    for load in loads[2:]:
        load.start()

    def pair_arrives(source, landing, index):
        to_pair(source, landing, index).wait_recv()

    loads[0].wait()
    loads[1].wait()
    group = math.lcm(32, tall)
    for first in range(0, features, group):

        def spread_signs(column, carry, first=first):
            lanes = pl.ds(pl.multiple_of(column * 128, 128), 128)
            weight = wts[pl.ds(first, group), lanes].astype(jnp.float32)
            shift = lax.broadcasted_iota(jnp.int32, (32, 128), 0)
            words = []
            for word in range(first // 32, (first + group) // 32):
                packed = jnp.broadcast_to(sig[pl.ds(word, 1), lanes], (32, 128))
                words.append((1 - 2 * jnp.bitwise_and(jnp.right_shift(packed, shift), 1)).astype(jnp.float32))
            probe = jnp.concatenate(words, axis=0)
            for part in range(group // tall):
                low = slice(part * tall, part * tall + per)
                high = slice(part * tall + per, (part + 1) * tall)
                both = [jnp.where(core == 0, matrix[low], matrix[high]) for matrix in (weight, probe)]
                stacked[first // tall + part, :, lanes] = jnp.concatenate(both, axis=0).astype(jnp.bfloat16)
            return carry

        lax.fori_loop(0, width // 128, spread_signs, 0)

    own_load.wait()
    tile = chips // 2
    last_dims = (((1,), (1,)), ((), ()))

    def differ(side):
        def one_chip(chip, carry):
            rows = pl.ds(pl.multiple_of(chip * tall, tall), tall)
            gap = res[side, rows].astype(jnp.float32) - tar[side, rows].astype(jnp.float32)
            apart[side, chip] = jnp.where(core == 0, gap[:per], gap[per:])
            return carry

        lax.fori_loop(0, chips, one_chip, 0)

    def forward(shard, side, pieces, slot):
        token_rows = span(shard, side)
        columns_of = pl.ds(pl.multiple_of(shard * tokens, tokens), tokens)

        def one_tile(t, carry):
            rows = pl.ds(pl.multiple_of(t * tile, tile), tile)
            total = None
            for start, size in pieces:
                term = lax.dot_general(
                    stacked[rows, :, pl.ds(start, size)].reshape(tile * tall, size),
                    hid[token_rows, pl.ds(start, size)],
                    last_dims,
                    preferred_element_type=jnp.float32,
                )
                total = term if total is None else total + term
            total = total.reshape(tile, tall, tokens)
            if pieces[0][0] > 0:
                total = total + acc[slot, rows]
            if pieces[-1][0] + pieces[-1][1] < width:
                acc[slot, rows] = total
                return carry
            misfit = total[:, :per] + apart[side, rows, :, columns_of]
            tangent = total[:, per:]
            inverse = lax.rsqrt(1.0 + misfit * misfit)
            slopes = misfit * inverse
            bends = tangent * (inverse * inverse * inverse)
            joined[t, ..., token_rows] = (
                jnp.concatenate([slopes, bends], axis=1).astype(jnp.bfloat16).reshape(*joined.shape[1:-1], tokens)
            )
            return carry

        lax.fori_loop(0, chips // tile, one_tile, 0)

    loads[4].wait()
    loads[5].wait()
    differ(core)
    with jax.named_scope("own"):
        forward(my_shard, core, [(0, width)], 0)
    pair_arrives(resid, res.at[1 - core], 1)
    pair_arrives(target, tar.at[1 - core], 2)
    differ(1 - core)
    pair_arrives(hidden, hid.at[span(my_shard, 1 - core)], 0)
    with jax.named_scope("pair"):
        forward(my_shard, 1 - core, [(0, width)], 0)
    loads[2].wait()
    loads[3].wait()

    def relay(shard, side, away, piece):
        where = hid.at[span(shard, side), pl.ds(*cuts[piece])]
        return pltpu.make_async_remote_copy(
            src_ref=where,
            dst_ref=where,
            send_sem=fwd_send.at[away - 1],
            recv_sem=fwd_recv.at[(away - 1) * len(cuts) + piece],
            device_id=device_of(1),
            device_id_type=MESH,
        )

    for piece, cut in enumerate(cuts):
        for away in range(1, shards):
            source = (my_shard + shards - away) % shards
            arriving = pltpu.make_async_remote_copy(
                src_ref=hidden.at[:, pl.ds(*cut)],
                dst_ref=hid.at[span(source, core), pl.ds(*cut)],
                send_sem=hid_send.at[away - 1],
                recv_sem=hid_recv.at[(away - 1) * len(cuts) + piece],
                device_id={"shard": source},
                device_id_type=MESH,
            )
            with jax.named_scope(f"x{piece}"):
                arriving.wait_recv()
            relay(source, core, away, piece).start()
            with jax.named_scope(f"f{piece}"):
                forward(source, core, [cut], (away - 1) * 2)
            with jax.named_scope(f"r{piece}"):
                relay(source, 1 - core, away, piece).wait_recv()
            with jax.named_scope(f"g{piece}"):
                forward(source, 1 - core, [cut], (away - 1) * 2 + 1)

    def sides(mask, group):
        return {bit: 1 - mine[bit] if mask >> bit & 1 else mine[bit] for bit in group}

    def remote(source, landing, send, recv, mask):
        return pltpu.make_async_remote_copy(
            src_ref=source,
            dst_ref=landing,
            send_sem=send,
            recv_sem=recv,
            device_id=device_of(mask),
            device_id_type=MESH,
        )

    stages = []
    gather_sems = {}
    for chunk, (scatter, gather) in enumerate(routes):
        open_bits, slot, level, found = list(range(1, bits)), 0, 0, []
        for group in scatter:
            after = [bit for bit in open_bits if bit not in group]
            size = 2 ** len(after)
            slots = {mask: slot + n * size for n, mask in enumerate(masks_of(group)[1:])}
            found.append((open_bits, after, slots, size, slot, slot + size * len(slots), level))
            open_bits, slot, level = after, slot + size * len(slots), level + size
        stages.append(found)
        for group in gather:
            for mask in masks_of(group)[1:]:
                gather_sems[chunk, mask] = len(gather_sems)

    def scatter_send(chunk, stage, mask):
        _, _, slots, size, _, _, _ = stages[chunk][stage]
        part = pl.ds(slots[mask], size)
        remote(sends.at[chunk, part], gots.at[chunk, part], rs_send.at[0], rs_recv.at[chunk, stage], mask).start()

    def scatter_wait(chunk, stage):
        _, _, slots, _, first, last, _ = stages[chunk][stage]
        part = pl.ds(first, last - first)
        mask = next(iter(slots))
        remote(sends.at[chunk, part], gots.at[chunk, part], rs_send.at[0], rs_recv.at[chunk, stage], mask).wait_recv()

    def landed(chunk, stage, index):
        _, _, slots, _, _, _, level = stages[chunk][stage]
        total = prod[chunk, level + index]
        for slot in slots.values():
            total = total + gots[chunk, slot + index].astype(jnp.float32)
        return total

    def backward(chunk):
        columns = pl.ds(chunk * CHUNK, CHUNK)
        group = routes[chunk][0][0]
        _, after, slots, size, _, _, level = stages[chunk][0]
        total = jnp.dot(
            joined[...].reshape(chips * tall, joined.shape[-1]),
            hid[:, columns],
            preferred_element_type=jnp.float32,
        ).reshape(*joined.shape[:-1], CHUNK)
        for mask in reversed(masks_of(group)):
            part = total
            for bit in sorted(group):
                axis = bits - 1 - bit
                low, high = (lax.index_in_dim(part, value, axis) for value in range(2))
                part = jnp.where((mine[bit] == 0) == (mask >> bit & 1 == 0), low, high)
            part = part.reshape(size, tall, CHUNK)
            if mask:
                sends[chunk, pl.ds(slots[mask], size)] = part.astype(jnp.bfloat16)
                scatter_send(chunk, 0, mask)
            else:
                prod[chunk, pl.ds(level, size)] = part

    def fold(chunk, stage):
        group = routes[chunk][0][stage]
        before, after, slots, size, _, _, level = stages[chunk][stage]
        for mask in reversed(masks_of(group)):
            for spot in range(size):
                values = sides(mask, group)
                values.update({bit: spot // 2**i % 2 for i, bit in enumerate(after)})
                index = sum(values[bit] * 2**i for i, bit in enumerate(before))
                total = landed(chunk, stage - 1, index)
                if mask:
                    sends[chunk, slots[mask] + spot] = total.astype(jnp.bfloat16)
                else:
                    prod[chunk, level + spot] = total
            if mask:
                scatter_send(chunk, stage, mask)

    def step_rows(chunk):
        first_fix = 1.0 - beta_one**OPT_STEP
        second_fix = 1.0 - beta_two**OPT_STEP
        here = tuple(reversed(mine))
        sums = landed(chunk, len(routes[chunk][0]) - 1, 0) * scaling
        fresh = []
        for part in range(CHUNK // 128):
            total = sums[:, part * 128 : (part + 1) * 128]
            rows = pl.ds(chunk * (CHUNK // 128) + part, per, stride=width // 128)
            first = beta_one * m_in[rows, :] + (1.0 - beta_one) * total[:per]
            second = beta_two * v_in[rows, :] + (1.0 - beta_two) * total[per:] * total[per:]
            m_out[rows, :] = first
            v_out[rows, :] = second
            update = first / first_fix / (jnp.sqrt(second / second_fix) + epsilon)
            weight = stacked[me // 2, :, pl.ds(chunk * CHUNK + part * 128, 128)].astype(jnp.float32)[:per]
            fresh.append(weight - learn_rate * update)
        half = len(fresh) // 2
        for part in range(half):
            both = jnp.concatenate([fresh[part], fresh[half + part]], axis=0)
            packs[(chunk, *here, slice(None), pl.ds(part * 128, 128))] = both.astype(jnp.bfloat16)

    def gathered(chunk, stage, mask):
        gather = routes[chunk][1]
        have = [bit for group in gather[:stage] for bit in group]
        values = sides(mask, range(bits))
        return packs.at[(chunk, *(slice(None) if bit in have else values[bit] for bit in reversed(range(bits))))]

    def gather_copy(chunk, stage, mask, arriving):
        where = gathered(chunk, stage, mask if arriving else 0)
        return remote(where, where, ag_send.at[0], ag_recv.at[gather_sems[chunk, mask]], mask)

    def lay_out(chunk):
        half = CHUNK // 2
        for pair in range(chips):
            spot = tuple(pair // 2**b % 2 for b in reversed(range(bits - 1)))
            even = packs[(chunk, *spot, 0)].astype(jnp.float32)
            odd = packs[(chunk, *spot, 1)].astype(jnp.float32)
            rows = pl.ds(pair * tall, tall)
            for side in range(2):
                part = slice(side * per, (side + 1) * per)
                both = jnp.concatenate([even[part], odd[part]], axis=0)
                w_asm[rows, pl.ds(chunk * CHUNK + side * half, half)] = both.astype(jnp.bfloat16)

    reached = [0] * len(routes)
    for chunk in order:
        scatter, gather = routes[chunk]
        step = reached[chunk]
        reached[chunk] += 1
        if step == 0:
            with jax.named_scope(f"b{chunk}"):
                backward(chunk)
            continue
        turn = step - len(scatter)
        with jax.named_scope(f"w{chunk}_{step}"):
            if turn <= 0:
                scatter_wait(chunk, step - 1)
            else:
                for mask in masks_of(gather[turn - 1])[1:]:
                    gather_copy(chunk, turn - 1, mask, True).wait_recv()
        with jax.named_scope(f"k{chunk}_{step}"):
            if turn < 0:
                fold(chunk, step)
            elif turn == 0:
                step_rows(chunk)
            if 0 <= turn < len(gather):
                for mask in reversed(masks_of(gather[turn])[1:]):
                    gather_copy(chunk, turn, mask, False).start()
            elif turn == len(gather):
                lay_out(chunk)
    assert all(done == len(a) + len(b) + 1 for done, (a, b) in zip(reached, routes))

    with jax.named_scope("ends"):
        for copy in pair_sends:
            copy.wait_send()
        whole = hid.at[span(my_shard, core)]
        for away in range(1, shards):
            remote(hidden, whole, hid_send.at[away - 1], hid_recv.at[0], 1).wait_send()
            remote(whole, whole, fwd_send.at[away - 1], fwd_recv.at[0], 1).wait_send()
        remote(sends, gots, rs_send.at[0], rs_recv.at[0, 0], 1).wait_send()
        sent = packs.reshape(len(routes), 2**bits, *packs.shape[-2:]).at[:, pl.ds(0, 2**bits - 1)]
        remote(sent, sent, ag_send.at[0], ag_recv.at[0], 1).wait_send()


def copy_out(*refs):
    sources, results, sems = refs[:3], refs[3:6], refs[6]
    copies = [pltpu.make_async_copy(a, b, sems.at[i]) for i, (a, b) in enumerate(zip(sources, results))]
    for copy in copies:
        copy.start()
    for copy in copies:
        copy.wait()


def write_out(results):
    return pl.pallas_call(
        copy_out,
        out_shape=tuple(jax.ShapeDtypeStruct(r.shape, r.dtype) for r in results),
        in_specs=[pl.BlockSpec(memory_space=pl.ANY)] * 3,
        out_specs=(pl.BlockSpec(memory_space=pl.ANY),) * 3,
        scratch_shapes=[pltpu.SemaphoreType.DMA((3,))],
        compiler_params=pltpu.CompilerParams(vmem_limit_bytes=1024 * 1024, has_side_effects=True),
    )(*results)


def in_one_kernel(hidden, resid, target, w_out, signs, m_old, v_old):
    blocks, shards = lax.axis_size("dp"), lax.axis_size("shard")
    features, width = w_out.shape
    tokens = hidden.shape[0]
    per = features // blocks
    tall = 2 * per
    chips = blocks // 2
    bits = blocks.bit_length() - 1
    chunks = width // CHUNK
    routes = routes_of(bits)
    waits = sum(len(masks_of(group)) - 1 for _, gather in routes for group in gather)
    half = width // 2
    cuts = [(0, half), (half, half - 2 * CHUNK), (width - 2 * CHUNK, CHUNK), (width - CHUNK, CHUNK)]
    scaling = 1.0 / math.sqrt(tokens * blocks * shards)
    bf16, f32 = jnp.bfloat16, jnp.float32
    dma = pltpu.SemaphoreType.DMA
    anywhere = pl.BlockSpec(memory_space=pl.ANY)
    results = pl.pallas_call(
        functools.partial(kernel, routes, ORDER, cuts, scaling),
        out_shape=(
            pltpu.VMEM(w_out.shape, bf16),
            pltpu.VMEM(m_old.shape, f32),
            pltpu.VMEM(v_old.shape, f32),
        ),
        in_specs=[anywhere] * 7,
        out_specs=(pl.BlockSpec(memory_space=pltpu.VMEM),) * 3,
        scratch_shapes=[
            pltpu.VMEM((shards * 2 * tokens, width), bf16),
            pltpu.VMEM((2, *resid.shape), bf16),
            pltpu.VMEM((2, *target.shape), bf16),
            pltpu.VMEM(w_out.shape, bf16),
            pltpu.VMEM(signs.shape, jnp.int32),
            pltpu.VMEM(m_old.shape, f32),
            pltpu.VMEM(v_old.shape, f32),
            pltpu.VMEM((chips, tall, width), bf16),
            pltpu.VMEM((2, chips, per, shards * tokens), f32),
            pltpu.VMEM((*((2,) * (bits - 1)), tall, shards * 2 * tokens), bf16),
            pltpu.VMEM((2 * (shards - 1), chips, tall, tokens), f32),
            pltpu.VMEM((chunks, chips - 1, tall, CHUNK), f32),
            pltpu.VMEM((chunks, chips - 1, tall, CHUNK), bf16),
            pltpu.VMEM((chunks, chips - 1, tall, CHUNK), bf16),
            pltpu.VMEM((chunks, *((2,) * bits), tall, CHUNK // 2), bf16),
            dma((7,)),
            dma((3,)),
            dma((3,)),
            dma((shards - 1,)),
            dma(((shards - 1) * len(cuts),)),
            dma((shards - 1,)),
            dma(((shards - 1) * len(cuts),)),
            dma((1,)),
            dma((chunks, bits - 1)),
            dma((1,)),
            dma((waits,)),
        ],
        compiler_params=pltpu.CompilerParams(
            collective_id=0, has_side_effects=True, vmem_limit_bytes=54 * 1024 * 1024
        ),
    )(hidden, resid, target, w_out, signs, m_old, v_old)
    return write_out(results)


def fits(hidden, w_out):
    blocks, shards = lax.axis_size("dp"), lax.axis_size("shard")
    features, width = w_out.shape
    per = features // blocks
    return (
        shards > 1
        and blocks == 16
        and features % (blocks * 8) == 0
        and features % math.lcm(32, 2 * per) == 0
        and width == len(ROUTES) * CHUNK
        and hidden.shape[0] % 128 == 0
    )


def either(hidden, resid, target, w_out, signs, m_old, v_old):
    run = in_one_kernel if fits(hidden, w_out) else on_device
    return run(hidden, resid, target, w_out, signs, m_old, v_old)


def solution(mesh):
    return jax.shard_map(
        either,
        mesh=mesh,
        in_specs=(
            P(("dp", "shard"), None),
            P("shard", "dp"),
            P("shard", "dp"),
            P("shard", None),
            P("shard", None),
            P(("shard", "dp"), None),
            P(("shard", "dp"), None),
        ),
        out_specs=(P("shard", None), P(("shard", "dp"), None), P(("shard", "dp"), None)),
        check_vma=False,
    )
```

```python
import functools
import math

import jax
import jax.numpy as jnp
from jax import lax
from jax.experimental import pallas as pl
from jax.experimental.pallas import tpu as pltpu
from jax.sharding import PartitionSpec as P

OPT_STEP = 10


beta_one = 0.9
beta_two = 0.999
learn_rate = 0.15
epsilon = 0.0001


def unpack_signs(signs):
    shifts = jnp.arange(32, dtype=jnp.int32)
    bit_values = jnp.bitwise_and(jnp.right_shift(signs[:, None, :], shifts[None, :, None]), 1)
    return (1 - 2 * bit_values).reshape(signs.shape[0] * 32, signs.shape[1]).astype(jnp.bfloat16)


def on_device(hidden, resid, target, w_out, signs, m_old, v_old):
    features = w_out.shape[0]
    probes = unpack_signs(signs)
    gathered = lax.all_gather(hidden, "shard", axis=0, tiled=True)
    stacked = jnp.concatenate([w_out, probes], axis=0)
    forward = lax.dot_general(
        stacked, gathered, (((1,), (1,)), ((), ())), preferred_element_type=jnp.float32
    )
    output = forward[:features]
    tangent = forward[features:]
    misfit = resid.astype(jnp.float32) + output - target.astype(jnp.float32)
    spread = 1.0 + misfit * misfit
    rooted = jnp.sqrt(spread)
    slopes = (misfit / rooted).astype(jnp.bfloat16)
    bends = (tangent / (spread * rooted)).astype(jnp.bfloat16)
    joined = jnp.concatenate([slopes, bends], axis=0)
    products = jnp.dot(joined, gathered, preferred_element_type=jnp.float32)
    grad_flat = products[:features].reshape(-1, 128)
    curve_flat = products[features:].reshape(-1, 128)
    replicas = lax.axis_size("dp")
    rows_each = grad_flat.shape[0] // replicas
    row_start = lax.axis_index("dp") * rows_each
    grad_mine, curve_mine = (
        lax.psum_scatter(grad_flat, "dp", scatter_dimension=0, tiled=True),
        lax.psum_scatter(curve_flat, "dp", scatter_dimension=0, tiled=True),
    )
    tokens_all = hidden.shape[0] * replicas * lax.axis_size("shard")
    scaling = 1.0 / math.sqrt(tokens_all)
    gradient = grad_mine * scaling
    curvature = curve_mine * scaling
    my_probes = lax.dynamic_slice_in_dim(probes.reshape(-1, 128), row_start, rows_each, 0)
    diag_est = my_probes.astype(jnp.float32) * curvature
    new_m = beta_one * m_old + (1.0 - beta_one) * gradient
    new_v = beta_two * v_old + (1.0 - beta_two) * diag_est * diag_est
    first_fix = 1.0 - beta_one**OPT_STEP
    second_fix = 1.0 - beta_two**OPT_STEP
    update = new_m / first_fix / (jnp.sqrt(new_v / second_fix) + epsilon)
    own_rows = lax.dynamic_slice_in_dim(w_out.reshape(-1, 128), row_start, rows_each, 0)
    fresh_rows = (own_rows.astype(jnp.float32) - learn_rate * update).astype(jnp.bfloat16)
    new_w = lax.all_gather(fresh_rows, "dp", axis=0, tiled=True).reshape(w_out.shape)
    return (new_w, new_m, new_v)


MESH = pl.DeviceIdType.MESH
CHUNK = 256


ROUTES = [
    [[2, 3], [1], [-1], [1], [4], [5]],
    [[1], [2, 3], [-1], [3], [2], [1]],
    [[1], [2, 3], [-1], [4], [5], [1]],
    [[1], [2, 3], [-1], [4], [5], [1]],
    [[2], [1], [3], [-1], [2, 3], [1]],
    [[1], [4], [5], [-1], [3], [2], [1]],
    [[1], [2, 3], [-1], [3], [2], [1]],
    [[1], [4], [5], [-1], [3], [1], [2]],
    [[1], [4], [5], [-1], [3], [1], [2]],
    [[1], [4], [5], [-1], [2, 3], [1]],
]
ORDER = [
    0, 2, 4, 6, 8, 1, 0, 2, 3, 4, 1, 5, 2, 6, 3, 1, 5, 7, 2, 6, 3, 8, 1, 5,
    7, 9, 2, 0, 6, 3, 8, 4, 5, 1, 7, 9, 1, 6, 2, 0, 8, 2, 3, 4, 5, 3, 7, 6,
    9, 0, 6, 8, 5, 4, 7, 5, 9, 8, 4, 0, 7, 4, 9, 0, 7, 8, 9, 8,
]

LINE, ACROSS = 4, 5


def masks_of(group):
    masks = [0]
    for bit in group:
        masks = masks + [mask | 1 << bit for mask in masks]
    return masks


def masks_in(group):
    if group[0] == ACROSS:
        return [8, 12]
    return [4] if group[0] == LINE else masks_of(group)[1:]


def routes_of():
    ends = [route.index([-1]) for route in ROUTES]
    return [(route[:end], route[end + 1 :] + [[0]]) for route, end in zip(ROUTES, ends)]


def kernel(
    routes, order, cuts, scaling,
    hidden, resid, target, w_out, signs, m_old, v_old,
    w_asm, m_out, v_out,
    hid, res, tar, wts, sig, m_in, v_in,
    stacked, apart, joined, acc, prod, sends, gots, packs,
    load_sem, pair_send, pair_recv, hid_send, hid_recv, fwd_send, fwd_recv, rs_send, rs_recv, ag_send, ag_recv,
):
    width = hid.shape[1]
    tokens = hidden.shape[0]
    shards = hid.shape[0] // tokens // 2
    chips, tall, _ = stacked.shape
    per = tall // 2
    features = chips * tall
    bits = (2 * chips).bit_length() - 1
    me = lax.axis_index("dp")
    my_shard = lax.axis_index("shard")
    mine = [me // 2**bit % 2 for bit in range(bits)]
    core = mine[0]

    def device_of(mask):
        return {"dp": me + sum((1 - 2 * mine[bit]) * 2**bit for bit in range(bits) if mask >> bit & 1)}

    def span(shard, side):
        return pl.ds(pl.multiple_of((shard * 2 + side) * tokens, tokens), tokens)

    own_load = pltpu.make_async_copy(hidden, hid.at[span(my_shard, core)], load_sem.at[0])
    loads = [
        pltpu.make_async_copy(w_out, wts, load_sem.at[1]),
        pltpu.make_async_copy(signs, sig, load_sem.at[2]),
        pltpu.make_async_copy(m_old, m_in, load_sem.at[3]),
        pltpu.make_async_copy(v_old, v_in, load_sem.at[4]),
        pltpu.make_async_copy(resid, res.at[core], load_sem.at[5]),
        pltpu.make_async_copy(target, tar.at[core], load_sem.at[6]),
    ]
    for load in loads[:2]:
        load.start()
    own_load.start()

    barrier = pltpu.get_barrier_semaphore()
    meets = {mask for route in routes for stages in route for group in stages for mask in masks_in(group)}
    for mask in sorted(meets):
        pl.semaphore_signal(barrier, inc=1, device_id=device_of(mask), device_id_type=MESH)
    for away in range(1, shards):
        other = (my_shard + away) % shards
        pl.semaphore_signal(barrier, inc=1, device_id={"shard": other}, device_id_type=MESH)
    pl.semaphore_wait(barrier, len(meets) + shards - 1)

    for piece, (start, size) in enumerate(cuts):
        for away in range(1, shards):
            copy = pltpu.make_async_remote_copy(
                src_ref=hidden.at[:, pl.ds(start, size)],
                dst_ref=hid.at[span(my_shard, core), pl.ds(start, size)],
                send_sem=hid_send.at[away - 1],
                recv_sem=hid_recv.at[(away - 1) * len(cuts) + piece],
                device_id={"shard": (my_shard + away) % shards},
                device_id_type=MESH,
            )
            copy.start()

    def to_pair(source, landing, index):
        return pltpu.make_async_remote_copy(
            src_ref=source,
            dst_ref=landing,
            send_sem=pair_send.at[index],
            recv_sem=pair_recv.at[index],
            device_id=device_of(1),
            device_id_type=MESH,
        )

    pair_sends = [
        to_pair(hidden, hid.at[span(my_shard, core)], 0),
        to_pair(resid, res.at[core], 1),
        to_pair(target, tar.at[core], 2),
    ]
    for copy in pair_sends:
        copy.start()
    for load in loads[2:]:
        load.start()

    def pair_arrives(source, landing, index):
        to_pair(source, landing, index).wait_recv()

    loads[0].wait()
    loads[1].wait()
    group = math.lcm(32, tall)
    for first in range(0, features, group):

        def spread_signs(column, carry, first=first):
            lanes = pl.ds(pl.multiple_of(column * 128, 128), 128)
            weight = wts[pl.ds(first, group), lanes].astype(jnp.float32)
            shift = lax.broadcasted_iota(jnp.int32, (32, 128), 0)
            words = []
            for word in range(first // 32, (first + group) // 32):
                packed = jnp.broadcast_to(sig[pl.ds(word, 1), lanes], (32, 128))
                words.append((1 - 2 * jnp.bitwise_and(jnp.right_shift(packed, shift), 1)).astype(jnp.float32))
            probe = jnp.concatenate(words, axis=0)
            for part in range(group // tall):
                low = slice(part * tall, part * tall + per)
                high = slice(part * tall + per, (part + 1) * tall)
                both = [jnp.where(core == 0, matrix[low], matrix[high]) for matrix in (weight, probe)]
                stacked[first // tall + part, :, lanes] = jnp.concatenate(both, axis=0).astype(jnp.bfloat16)
            return carry

        lax.fori_loop(0, width // 128, spread_signs, 0)

    own_load.wait()
    tile = chips // 2
    last_dims = (((1,), (1,)), ((), ()))

    def differ(side):
        def one_chip(chip, carry):
            rows = pl.ds(pl.multiple_of(chip * tall, tall), tall)
            gap = res[side, rows].astype(jnp.float32) - tar[side, rows].astype(jnp.float32)
            apart[side, chip] = jnp.where(core == 0, gap[:per], gap[per:])
            return carry

        lax.fori_loop(0, chips, one_chip, 0)

    def forward(shard, side, pieces, slot):
        token_rows = span(shard, side)
        columns_of = pl.ds(pl.multiple_of(shard * tokens, tokens), tokens)

        def one_tile(t, carry):
            rows = pl.ds(pl.multiple_of(t * tile, tile), tile)
            total = None
            for start, size in pieces:
                term = lax.dot_general(
                    stacked[rows, :, pl.ds(start, size)].reshape(tile * tall, size),
                    hid[token_rows, pl.ds(start, size)],
                    last_dims,
                    preferred_element_type=jnp.float32,
                )
                total = term if total is None else total + term
            total = total.reshape(tile, tall, tokens)
            if pieces[0][0] > 0:
                total = total + acc[slot, rows]
            if pieces[-1][0] + pieces[-1][1] < width:
                acc[slot, rows] = total
                return carry
            misfit = total[:, :per] + apart[side, rows, :, columns_of]
            tangent = total[:, per:]
            inverse = lax.rsqrt(1.0 + misfit * misfit)
            slopes = misfit * inverse
            bends = tangent * (inverse * inverse * inverse)
            joined[t, ..., token_rows] = (
                jnp.concatenate([slopes, bends], axis=1).astype(jnp.bfloat16).reshape(*joined.shape[1:-1], tokens)
            )
            return carry

        lax.fori_loop(0, chips // tile, one_tile, 0)

    loads[4].wait()
    loads[5].wait()
    differ(core)
    with jax.named_scope("own"):
        forward(my_shard, core, [(0, width)], 0)
    pair_arrives(resid, res.at[1 - core], 1)
    pair_arrives(target, tar.at[1 - core], 2)
    differ(1 - core)
    pair_arrives(hidden, hid.at[span(my_shard, 1 - core)], 0)
    with jax.named_scope("pair"):
        forward(my_shard, 1 - core, [(0, width)], 0)
    loads[2].wait()
    loads[3].wait()

    def relay(shard, side, away, piece):
        where = hid.at[span(shard, side), pl.ds(*cuts[piece])]
        return pltpu.make_async_remote_copy(
            src_ref=where,
            dst_ref=where,
            send_sem=fwd_send.at[away - 1],
            recv_sem=fwd_recv.at[(away - 1) * len(cuts) + piece],
            device_id=device_of(1),
            device_id_type=MESH,
        )

    for piece, cut in enumerate(cuts):
        for away in range(1, shards):
            source = (my_shard + shards - away) % shards
            arriving = pltpu.make_async_remote_copy(
                src_ref=hidden.at[:, pl.ds(*cut)],
                dst_ref=hid.at[span(source, core), pl.ds(*cut)],
                send_sem=hid_send.at[away - 1],
                recv_sem=hid_recv.at[(away - 1) * len(cuts) + piece],
                device_id={"shard": source},
                device_id_type=MESH,
            )
            with jax.named_scope(f"x{piece}"):
                arriving.wait_recv()
            relay(source, core, away, piece).start()
            with jax.named_scope(f"f{piece}"):
                forward(source, core, [cut], (away - 1) * 2)
            with jax.named_scope(f"r{piece}"):
                relay(source, 1 - core, away, piece).wait_recv()
            with jax.named_scope(f"g{piece}"):
                forward(source, 1 - core, [cut], (away - 1) * 2 + 1)

    def sides(mask, group):
        return {bit: 1 - mine[bit] if mask >> bit & 1 else mine[bit] for bit in group}

    def remote(source, landing, send, recv, mask):
        return pltpu.make_async_remote_copy(
            src_ref=source,
            dst_ref=landing,
            send_sem=send,
            recv_sem=recv,
            device_id=device_of(mask),
            device_id_type=MESH,
        )

    outer = mine[2] == mine[3]
    inner = mine[2] != mine[3]
    stages, scatter_sems, gather_sems = [], {}, {}
    for chunk, (scatter, gather) in enumerate(routes):
        open_bits, out, into, level, found = list(range(1, bits)), 0, 0, 0, []
        for stage, group in enumerate(scatter):
            gone = [2, 3] if group[0] in (LINE, ACROSS) else group
            after = [bit for bit in open_bits if bit not in gone]
            size = 2 ** len(after)
            if group[0] == LINE:
                pieces, kept = {"far": 2, "near": 1}, 3
            elif group[0] == ACROSS:
                pieces, kept = {8: 1, 12: 1}, 0
            else:
                pieces, kept = {mask: 1 for mask in masks_of(group)[1:]}, 1
            info = {"before": open_bits, "after": after, "size": size, "level": level, "out": {}, "into": {}}
            for name, count in pieces.items():
                info["out"][name] = out
                info["into"][name] = into
                out += count * size
                into += count * size if group[0] != ACROSS else 0
            if group[0] == ACROSS:
                into += size
                info["level"] = found[-1]["level"]
            info["last"] = into
            names = ("far", "near") if group[0] == LINE else ("all",)
            for name in names:
                scatter_sems[chunk, stage, name] = len(scatter_sems)
            level += kept * size
            open_bits = after
            found.append(info)
        stages.append(found)
        for stage, group in enumerate(gather):
            for mask in masks_in(group)[:1] if group[0] == ACROSS else masks_in(group):
                gather_sems[chunk, stage, mask] = len(gather_sems)

    def scatter_copy(chunk, stage, name, mask, begin, into, size):
        return remote(
            sends.at[chunk, pl.ds(begin, size)],
            gots.at[chunk, pl.ds(into, size)],
            rs_send.at[0],
            rs_recv.at[scatter_sems[chunk, stage, name]],
            mask,
        )

    def scatter_send(chunk, stage, mask, name="all", slot=None, count=1):
        info = stages[chunk][stage]
        slot = mask if slot is None else slot
        scatter_copy(chunk, stage, name, mask, info["out"][slot], info["into"][slot], count * info["size"]).start()

    def scatter_wait(chunk, stage, name="all"):
        info, group = stages[chunk][stage], routes[chunk][0][stage]
        if group[0] == LINE:
            first, size = info["into"][name], info["size"] * (2 if name == "far" else 1)
        else:
            first = min(info["into"].values())
            size = info["last"] - first
        scatter_copy(chunk, stage, name, 4, 0, first, size).wait_recv()

    def landed(chunk, stage, index):
        info = stages[chunk][stage]
        total = prod[chunk, info["level"] + index]
        slots = sorted(set(info["into"].values()))
        if routes[chunk][0][stage][0] == ACROSS:
            slots = slots + [stages[chunk][stage - 1]["into"]["near"]]
        for slot in slots:
            total = total + gots[chunk, slot + index].astype(jnp.float32)
        return total

    def hand_out(chunk, stage, blocks_for):
        info, group = stages[chunk][stage], routes[chunk][0][stage]
        size = info["size"]

        def put(mask, bits_of, slot):
            sends[chunk, pl.ds(slot, size)] = blocks_for(mask, bits_of).astype(jnp.bfloat16)

        if group[0] != LINE:
            for mask in reversed(masks_of(group)):
                if mask:
                    put(mask, group, info["out"][mask])
                    scatter_send(chunk, stage, mask)
                else:
                    prod[chunk, pl.ds(info["level"], size)] = blocks_for(0, group)
            return
        far, near = info["out"]["far"], info["out"]["near"]

        @pl.when(outer)
        def _():
            put(12, [2, 3], far)
            put(8, [2, 3], far + size)
            scatter_send(chunk, stage, 4, "far", "far", 2)

        put(4, [2, 3], near)
        scatter_send(chunk, stage, 4, "near", "near")
        prod[chunk, pl.ds(info["level"], size)] = blocks_for(0, [2, 3])

        @pl.when(inner)
        def _():
            prod[chunk, pl.ds(info["level"] + size, size)] = blocks_for(8, [2, 3])
            prod[chunk, pl.ds(info["level"] + 2 * size, size)] = blocks_for(12, [2, 3])

    def backward(lead):
        pair = lead // 2
        total = jnp.dot(
            joined[...].reshape(chips * tall, joined.shape[-1]),
            hid[:, pl.ds(pair * 2 * CHUNK, 2 * CHUNK)],
            preferred_element_type=jnp.float32,
        ).reshape(*joined.shape[:-1], 2 * CHUNK)
        for half in (lead % 2, 1 - lead % 2):

            def blocks_for(mask, group, half=half):
                part = total[..., half * CHUNK : (half + 1) * CHUNK]
                for bit in sorted(group):
                    axis = bits - 1 - bit
                    low, high = (lax.index_in_dim(part, value, axis) for value in range(2))
                    part = jnp.where((mine[bit] == 0) == (mask >> bit & 1 == 0), low, high)
                return part.reshape(-1, tall, CHUNK)

            hand_out(pair * 2 + half, 0, blocks_for)

    def fold(chunk, stage):
        info, group = stages[chunk][stage], routes[chunk][0][stage]
        size = info["size"]
        if group[0] == ACROSS:

            @pl.when(inner)
            def _():
                scatter_wait(chunk, stage - 1, "far")
                line = stages[chunk][stage - 1]
                for mask, kept, slot in ((8, size, 0), (12, 2 * size, size)):
                    held = prod[chunk, pl.ds(line["level"] + kept, size)]
                    came = gots[chunk, pl.ds(line["into"]["far"] + slot, size)].astype(jnp.float32)
                    sends[chunk, pl.ds(info["out"][mask], size)] = (held + came).astype(jnp.bfloat16)
                    scatter_send(chunk, stage, mask)

            return

        def blocks_for(mask, group):
            found = []
            for spot in range(size):
                values = sides(mask, group)
                values.update({bit: spot // 2**i % 2 for i, bit in enumerate(info["after"])})
                index = sum(values[bit] * 2**i for i, bit in enumerate(info["before"]))
                found.append(landed(chunk, stage - 1, index))
            return jnp.stack(found)

        hand_out(chunk, stage, blocks_for)

    def step_rows(chunk):
        first_fix = 1.0 - beta_one**OPT_STEP
        second_fix = 1.0 - beta_two**OPT_STEP
        here = tuple(reversed(mine))
        sums = landed(chunk, len(routes[chunk][0]) - 1, 0) * scaling
        fresh = []
        for part in range(CHUNK // 128):
            total = sums[:, part * 128 : (part + 1) * 128]
            rows = pl.ds(chunk * (CHUNK // 128) + part, per, stride=width // 128)
            first = beta_one * m_in[rows, :] + (1.0 - beta_one) * total[:per]
            second = beta_two * v_in[rows, :] + (1.0 - beta_two) * total[per:] * total[per:]
            m_out[rows, :] = first
            v_out[rows, :] = second
            update = first / first_fix / (jnp.sqrt(second / second_fix) + epsilon)
            weight = stacked[me // 2, :, pl.ds(chunk * CHUNK + part * 128, 128)].astype(jnp.float32)[:per]
            fresh.append(weight - learn_rate * update)
        half = len(fresh) // 2
        for part in range(half):
            both = jnp.concatenate([fresh[part], fresh[half + part]], axis=0)
            packs[(chunk, *here, slice(None), pl.ds(part * 128, 128))] = both.astype(jnp.bfloat16)

    def gathered(chunk, stage, mask):
        gather = routes[chunk][1]
        have = [bit for group in gather[:stage] for bit in (group if group[0] < LINE else [group[0] - 2])]
        values = sides(mask, range(bits))
        return packs.at[(chunk, *(slice(None) if bit in have else values[bit] for bit in reversed(range(bits))))]

    def gather_start(chunk, stage):
        group = routes[chunk][1][stage]
        where = gathered(chunk, stage, 0)
        if group[0] == ACROSS:
            sem = ag_recv.at[gather_sems[chunk, stage, 8]]

            @pl.when(inner)
            def _():
                for mask in (8, 12):
                    remote(where, where, ag_send.at[1], sem, mask).start()

            return
        for mask in reversed(masks_in(group)):
            remote(where, where, ag_send.at[0], ag_recv.at[gather_sems[chunk, stage, mask]], mask).start()

    def gather_wait(chunk, stage):
        group = routes[chunk][1][stage]
        for mask in [8] if group[0] == ACROSS else masks_in(group):
            where = gathered(chunk, stage, mask)
            remote(where, where, ag_send.at[0], ag_recv.at[gather_sems[chunk, stage, mask]], mask).wait_recv()

    def lay_out(chunk):
        half = CHUNK // 2
        for pair in range(chips):
            spot = tuple(pair // 2**b % 2 for b in reversed(range(bits - 1)))
            even = packs[(chunk, *spot, 0)].astype(jnp.float32)
            odd = packs[(chunk, *spot, 1)].astype(jnp.float32)
            rows = pl.ds(pair * tall, tall)
            for side in range(2):
                part = slice(side * per, (side + 1) * per)
                both = jnp.concatenate([even[part], odd[part]], axis=0)
                w_asm[rows, pl.ds(chunk * CHUNK + side * half, half)] = both.astype(jnp.bfloat16)

    reached = [0] * len(routes)
    for chunk in order:
        scatter, gather = routes[chunk]
        step = reached[chunk]
        if step == 0:
            with jax.named_scope(f"b{chunk // 2}"):
                backward(chunk)
            reached[chunk] = reached[chunk ^ 1] = 1
            continue
        reached[chunk] += 1
        turn = step - len(scatter)
        with jax.named_scope(f"w{chunk}_{step}"):
            if turn <= 0:
                past = scatter[step - 1][0]
                if past == ACROSS:
                    scatter_wait(chunk, step - 2, "near")
                if past != LINE:
                    scatter_wait(chunk, step - 1)
            else:
                gather_wait(chunk, turn - 1)
        with jax.named_scope(f"k{chunk}_{step}"):
            if turn < 0:
                fold(chunk, step)
            elif turn == 0:
                step_rows(chunk)
            if 0 <= turn < len(gather):
                gather_start(chunk, turn)
            elif turn == len(gather):
                lay_out(chunk)
    assert all(done == len(a) + len(b) + 1 for done, (a, b) in zip(reached, routes))

    with jax.named_scope("ends"):
        for copy in pair_sends:
            copy.wait_send()
        whole = hid.at[span(my_shard, core)]
        for away in range(1, shards):
            remote(hidden, whole, hid_send.at[away - 1], hid_recv.at[0], 1).wait_send()
            remote(whole, whole, fwd_send.at[away - 1], fwd_recv.at[0], 1).wait_send()
        flat = sends.reshape(-1, *sends.shape[2:]).at[pl.ds(0, len(routes) * (chips - 1))]
        remote(flat, flat, rs_send.at[0], rs_recv.at[0], 1).wait_send()
        flat = packs.reshape(-1, *packs.shape[-2:])
        plain = across = 0
        for _, gather in routes:
            have = 1
            for group in gather:
                if group[0] == ACROSS:
                    across += 2 * have
                else:
                    plain += have * len(masks_in(group))
                have *= len(masks_of(group)) if group[0] < LINE else 2
        part = flat.at[pl.ds(0, plain)]
        remote(part, part, ag_send.at[0], ag_recv.at[0], 1).wait_send()
        if across:

            @pl.when(inner)
            def _():
                part = flat.at[pl.ds(0, across)]
                remote(part, part, ag_send.at[1], ag_recv.at[0], 1).wait_send()


def copy_out(*refs):
    sources, results, sems = refs[:3], refs[3:6], refs[6]
    copies = [pltpu.make_async_copy(a, b, sems.at[i]) for i, (a, b) in enumerate(zip(sources, results))]
    for copy in copies:
        copy.start()
    for copy in copies:
        copy.wait()


def write_out(results):
    return pl.pallas_call(
        copy_out,
        out_shape=tuple(jax.ShapeDtypeStruct(r.shape, r.dtype) for r in results),
        in_specs=[pl.BlockSpec(memory_space=pl.ANY)] * 3,
        out_specs=(pl.BlockSpec(memory_space=pl.ANY),) * 3,
        scratch_shapes=[pltpu.SemaphoreType.DMA((3,))],
        compiler_params=pltpu.CompilerParams(vmem_limit_bytes=1024 * 1024, has_side_effects=True),
    )(*results)


def in_one_kernel(hidden, resid, target, w_out, signs, m_old, v_old):
    blocks, shards = lax.axis_size("dp"), lax.axis_size("shard")
    features, width = w_out.shape
    tokens = hidden.shape[0]
    per = features // blocks
    tall = 2 * per
    chips = blocks // 2
    bits = blocks.bit_length() - 1
    chunks = width // CHUNK
    routes = routes_of()
    waits = sum(1 if group[0] >= LINE else len(masks_in(group)) for _, gather in routes for group in gather)
    lands = sum(2 if group[0] == LINE else 1 for scatter, _ in routes for group in scatter)
    half = width // 2
    cuts = [(0, half), (half, half - 2 * CHUNK), (width - 2 * CHUNK, CHUNK), (width - CHUNK, CHUNK)]
    scaling = 1.0 / math.sqrt(tokens * blocks * shards)
    bf16, f32 = jnp.bfloat16, jnp.float32
    dma = pltpu.SemaphoreType.DMA
    anywhere = pl.BlockSpec(memory_space=pl.ANY)
    results = pl.pallas_call(
        functools.partial(kernel, routes, ORDER, cuts, scaling),
        out_shape=(
            pltpu.VMEM(w_out.shape, bf16),
            pltpu.VMEM(m_old.shape, f32),
            pltpu.VMEM(v_old.shape, f32),
        ),
        in_specs=[anywhere] * 7,
        out_specs=(pl.BlockSpec(memory_space=pltpu.VMEM),) * 3,
        scratch_shapes=[
            pltpu.VMEM((shards * 2 * tokens, width), bf16),
            pltpu.VMEM((2, *resid.shape), bf16),
            pltpu.VMEM((2, *target.shape), bf16),
            pltpu.VMEM(w_out.shape, bf16),
            pltpu.VMEM(signs.shape, jnp.int32),
            pltpu.VMEM(m_old.shape, f32),
            pltpu.VMEM(v_old.shape, f32),
            pltpu.VMEM((chips, tall, width), bf16),
            pltpu.VMEM((2, chips, per, shards * tokens), f32),
            pltpu.VMEM((*((2,) * (bits - 1)), tall, shards * 2 * tokens), bf16),
            pltpu.VMEM((2 * (shards - 1), chips, tall, tokens), f32),
            pltpu.VMEM((chunks, chips, tall, CHUNK), f32),
            pltpu.VMEM((chunks, chips + 3, tall, CHUNK), bf16),
            pltpu.VMEM((chunks, chips + 1, tall, CHUNK), bf16),
            pltpu.VMEM((chunks, *((2,) * bits), tall, CHUNK // 2), bf16),
            dma((7,)),
            dma((3,)),
            dma((3,)),
            dma((shards - 1,)),
            dma(((shards - 1) * len(cuts),)),
            dma((shards - 1,)),
            dma(((shards - 1) * len(cuts),)),
            dma((1,)),
            dma((lands,)),
            dma((2,)),
            dma((waits,)),
        ],
        compiler_params=pltpu.CompilerParams(
            collective_id=0, has_side_effects=True, vmem_limit_bytes=54 * 1024 * 1024
        ),
    )(hidden, resid, target, w_out, signs, m_old, v_old)
    return write_out(results)


def fits(hidden, w_out):
    blocks, shards = lax.axis_size("dp"), lax.axis_size("shard")
    features, width = w_out.shape
    per = features // blocks
    return (
        shards > 1
        and blocks == 16
        and features % (blocks * 8) == 0
        and features % math.lcm(32, 2 * per) == 0
        and width == len(ROUTES) * CHUNK
        and len(ROUTES) % 2 == 0
        and hidden.shape[0] % 128 == 0
    )


def either(hidden, resid, target, w_out, signs, m_old, v_old):
    run = in_one_kernel if fits(hidden, w_out) else on_device
    return run(hidden, resid, target, w_out, signs, m_old, v_old)


def solution(mesh):
    return jax.shard_map(
        either,
        mesh=mesh,
        in_specs=(
            P(("dp", "shard"), None),
            P("shard", "dp"),
            P("shard", "dp"),
            P("shard", None),
            P("shard", None),
            P(("shard", "dp"), None),
            P(("shard", "dp"), None),
        ),
        out_specs=(P("shard", None), P(("shard", "dp"), None), P(("shard", "dp"), None)),
        check_vma=False,
    )
```

```python
import functools
import math

import jax
import jax.numpy as jnp
from jax import lax
from jax.experimental import pallas as pl
from jax.experimental.pallas import tpu as pltpu
from jax.sharding import PartitionSpec as P

OPT_STEP = 10


beta_one = 0.9
beta_two = 0.999
learn_rate = 0.15
epsilon = 0.0001


def unpack_signs(signs):
    shifts = jnp.arange(32, dtype=jnp.int32)
    bit_values = jnp.bitwise_and(jnp.right_shift(signs[:, None, :], shifts[None, :, None]), 1)
    return (1 - 2 * bit_values).reshape(signs.shape[0] * 32, signs.shape[1]).astype(jnp.bfloat16)


def on_device(hidden, resid, target, w_out, signs, m_old, v_old):
    features = w_out.shape[0]
    probes = unpack_signs(signs)
    gathered = lax.all_gather(hidden, "shard", axis=0, tiled=True)
    stacked = jnp.concatenate([w_out, probes], axis=0)
    forward = lax.dot_general(
        stacked, gathered, (((1,), (1,)), ((), ())), preferred_element_type=jnp.float32
    )
    output = forward[:features]
    tangent = forward[features:]
    misfit = resid.astype(jnp.float32) + output - target.astype(jnp.float32)
    spread = 1.0 + misfit * misfit
    rooted = jnp.sqrt(spread)
    slopes = (misfit / rooted).astype(jnp.bfloat16)
    bends = (tangent / (spread * rooted)).astype(jnp.bfloat16)
    joined = jnp.concatenate([slopes, bends], axis=0)
    products = jnp.dot(joined, gathered, preferred_element_type=jnp.float32)
    grad_flat = products[:features].reshape(-1, 128)
    curve_flat = products[features:].reshape(-1, 128)
    replicas = lax.axis_size("dp")
    rows_each = grad_flat.shape[0] // replicas
    row_start = lax.axis_index("dp") * rows_each
    grad_mine, curve_mine = (
        lax.psum_scatter(grad_flat, "dp", scatter_dimension=0, tiled=True),
        lax.psum_scatter(curve_flat, "dp", scatter_dimension=0, tiled=True),
    )
    tokens_all = hidden.shape[0] * replicas * lax.axis_size("shard")
    scaling = 1.0 / math.sqrt(tokens_all)
    gradient = grad_mine * scaling
    curvature = curve_mine * scaling
    my_probes = lax.dynamic_slice_in_dim(probes.reshape(-1, 128), row_start, rows_each, 0)
    diag_est = my_probes.astype(jnp.float32) * curvature
    new_m = beta_one * m_old + (1.0 - beta_one) * gradient
    new_v = beta_two * v_old + (1.0 - beta_two) * diag_est * diag_est
    first_fix = 1.0 - beta_one**OPT_STEP
    second_fix = 1.0 - beta_two**OPT_STEP
    update = new_m / first_fix / (jnp.sqrt(new_v / second_fix) + epsilon)
    own_rows = lax.dynamic_slice_in_dim(w_out.reshape(-1, 128), row_start, rows_each, 0)
    fresh_rows = (own_rows.astype(jnp.float32) - learn_rate * update).astype(jnp.bfloat16)
    new_w = lax.all_gather(fresh_rows, "dp", axis=0, tiled=True).reshape(w_out.shape)
    return (new_w, new_m, new_v)


MESH = pl.DeviceIdType.MESH
CHUNK = 256


ROUTES = [
    [[2, 3], [1], [-1], [1], [4], [5]],
    [[1], [2, 3], [-1], [3], [2], [1]],
    [[1], [2, 3], [-1], [4], [5], [1]],
    [[1], [2, 3], [-1], [4], [5], [1]],
    [[2], [1], [3], [-1], [2, 3], [1]],
    [[1], [4], [5], [-1], [3], [2], [1]],
    [[1], [2, 3], [-1], [3], [2], [1]],
    [[1], [4], [5], [-1], [3], [1], [2]],
    [[1], [4], [5], [-1], [3], [1], [2]],
    [[1], [4], [5], [-1], [2, 3], [1]],
]
ORDER = [
    0, 2, 4, 6, 8, 1, 0, 2, 3, 4, 1, 5, 2, 6, 3, 1, 5, 7, 2, 6, 3, 8, 1, 5,
    7, 9, 2, 0, 6, 3, 8, 4, 5, 1, 7, 9, 1, 6, 2, 0, 8, 2, 3, 4, 5, 3, 7, 6,
    9, 0, 6, 8, 5, 4, 7, 5, 9, 8, 4, 0, 7, 4, 9, 0, 7, 8, 9, 8,
]

LINE, ACROSS = 4, 5


def masks_of(group):
    masks = [0]
    for bit in group:
        masks = masks + [mask | 1 << bit for mask in masks]
    return masks


def masks_in(group):
    if group[0] == ACROSS:
        return [8, 12]
    return [4] if group[0] == LINE else masks_of(group)[1:]


def routes_of():
    ends = [route.index([-1]) for route in ROUTES]
    return [(route[:end], route[end + 1 :] + [[0]]) for route, end in zip(ROUTES, ends)]


def kernel(
    routes, order, cuts, scaling,
    hidden, resid, target, w_out, signs, m_old, v_old,
    w_asm, m_out, v_out,
    hid, res, tar, wts, sig, m_in, v_in,
    stacked, apart, joined, acc, prod, sends, gots, packs,
    load_sem, pair_send, pair_recv, hid_send, hid_recv, fwd_send, fwd_recv, rs_send, rs_recv, ag_send, ag_recv,
):
    width = hid.shape[1]
    tokens = hidden.shape[0]
    shards = hid.shape[0] // tokens // 2
    chips, tall, _ = stacked.shape
    per = tall // 2
    features = chips * tall
    bits = (2 * chips).bit_length() - 1
    me = lax.axis_index("dp")
    my_shard = lax.axis_index("shard")
    mine = [me // 2**bit % 2 for bit in range(bits)]
    core = mine[0]

    def device_of(mask):
        return {"dp": me + sum((1 - 2 * mine[bit]) * 2**bit for bit in range(bits) if mask >> bit & 1)}

    def span(shard, side):
        return pl.ds(pl.multiple_of((shard * 2 + side) * tokens, tokens), tokens)

    own_load = pltpu.make_async_copy(hidden, hid.at[span(my_shard, core)], load_sem.at[0])
    loads = [
        pltpu.make_async_copy(w_out, wts, load_sem.at[1]),
        pltpu.make_async_copy(signs, sig, load_sem.at[2]),
        pltpu.make_async_copy(m_old, m_in, load_sem.at[3]),
        pltpu.make_async_copy(v_old, v_in, load_sem.at[4]),
        pltpu.make_async_copy(resid, res.at[core], load_sem.at[5]),
        pltpu.make_async_copy(target, tar.at[core], load_sem.at[6]),
    ]
    own_load.start()
    for load in loads[:2]:
        load.start()

    barrier = pltpu.get_barrier_semaphore()
    meets = {mask for route in routes for stages in route for group in stages for mask in masks_in(group)}
    for mask in sorted(meets):
        pl.semaphore_signal(barrier, inc=1, device_id=device_of(mask), device_id_type=MESH)
    for away in range(1, shards):
        other = (my_shard + away) % shards
        pl.semaphore_signal(barrier, inc=1, device_id={"shard": other}, device_id_type=MESH)
    pl.semaphore_wait(barrier, len(meets) + shards - 1)

    own_load.wait()
    for piece, (start, size) in enumerate(cuts):
        for away in range(1, shards):
            copy = pltpu.make_async_remote_copy(
                src_ref=hid.at[span(my_shard, core), pl.ds(start, size)],
                dst_ref=hid.at[span(my_shard, core), pl.ds(start, size)],
                send_sem=hid_send.at[away - 1],
                recv_sem=hid_recv.at[(away - 1) * len(cuts) + piece],
                device_id={"shard": (my_shard + away) % shards},
                device_id_type=MESH,
            )
            copy.start()

    def to_pair(source, landing, index):
        return pltpu.make_async_remote_copy(
            src_ref=source,
            dst_ref=landing,
            send_sem=pair_send.at[index],
            recv_sem=pair_recv.at[index],
            device_id=device_of(1),
            device_id_type=MESH,
        )

    pair_sends = [
        to_pair(hidden, hid.at[span(my_shard, core)], 0),
        to_pair(resid, res.at[core], 1),
        to_pair(target, tar.at[core], 2),
    ]
    for copy in pair_sends:
        copy.start()
    for load in loads[2:]:
        load.start()

    def pair_arrives(source, landing, index):
        to_pair(source, landing, index).wait_recv()

    loads[0].wait()
    loads[1].wait()
    group = math.lcm(32, tall)
    for first in range(0, features, group):

        def spread_signs(column, carry, first=first):
            lanes = pl.ds(pl.multiple_of(column * 128, 128), 128)
            weight = wts[pl.ds(first, group), lanes].astype(jnp.float32)
            shift = lax.broadcasted_iota(jnp.int32, (32, 128), 0)
            words = []
            for word in range(first // 32, (first + group) // 32):
                packed = jnp.broadcast_to(sig[pl.ds(word, 1), lanes], (32, 128))
                words.append((1 - 2 * jnp.bitwise_and(jnp.right_shift(packed, shift), 1)).astype(jnp.float32))
            probe = jnp.concatenate(words, axis=0)
            for part in range(group // tall):
                low = slice(part * tall, part * tall + per)
                high = slice(part * tall + per, (part + 1) * tall)
                both = [jnp.where(core == 0, matrix[low], matrix[high]) for matrix in (weight, probe)]
                stacked[first // tall + part, :, lanes] = jnp.concatenate(both, axis=0).astype(jnp.bfloat16)
            return carry

        lax.fori_loop(0, width // 128, spread_signs, 0)

    tile = chips // 2
    last_dims = (((1,), (1,)), ((), ()))

    def differ(side):
        def one_chip(chip, carry):
            rows = pl.ds(pl.multiple_of(chip * tall, tall), tall)
            gap = res[side, rows].astype(jnp.float32) - tar[side, rows].astype(jnp.float32)
            apart[side, chip] = jnp.where(core == 0, gap[:per], gap[per:])
            return carry

        lax.fori_loop(0, chips, one_chip, 0)

    def forward(shard, side, pieces, slot):
        token_rows = span(shard, side)
        columns_of = pl.ds(pl.multiple_of(shard * tokens, tokens), tokens)

        def one_tile(t, carry):
            rows = pl.ds(pl.multiple_of(t * tile, tile), tile)
            total = None
            for start, size in pieces:
                term = lax.dot_general(
                    stacked[rows, :, pl.ds(start, size)].reshape(tile * tall, size),
                    hid[token_rows, pl.ds(start, size)],
                    last_dims,
                    preferred_element_type=jnp.float32,
                )
                total = term if total is None else total + term
            total = total.reshape(tile, tall, tokens)
            if pieces[0][0] > 0:
                total = total + acc[slot, rows]
            if pieces[-1][0] + pieces[-1][1] < width:
                acc[slot, rows] = total
                return carry
            misfit = total[:, :per] + apart[side, rows, :, columns_of]
            tangent = total[:, per:]
            inverse = lax.rsqrt(1.0 + misfit * misfit)
            slopes = misfit * inverse
            bends = tangent * (inverse * inverse * inverse)
            joined[t, ..., token_rows] = (
                jnp.concatenate([slopes, bends], axis=1).astype(jnp.bfloat16).reshape(*joined.shape[1:-1], tokens)
            )
            return carry

        lax.fori_loop(0, chips // tile, one_tile, 0, unroll=pieces[-1][1] <= CHUNK)

    loads[4].wait()
    loads[5].wait()
    differ(core)
    with jax.named_scope("own"):
        forward(my_shard, core, [(0, width)], 0)
    pair_arrives(resid, res.at[1 - core], 1)
    pair_arrives(target, tar.at[1 - core], 2)
    differ(1 - core)
    pair_arrives(hidden, hid.at[span(my_shard, 1 - core)], 0)
    with jax.named_scope("pair"):
        forward(my_shard, 1 - core, [(0, width)], 0)
    loads[2].wait()
    loads[3].wait()

    def relay(shard, side, away, piece):
        where = hid.at[span(shard, side), pl.ds(*cuts[piece])]
        return pltpu.make_async_remote_copy(
            src_ref=where,
            dst_ref=where,
            send_sem=fwd_send.at[away - 1],
            recv_sem=fwd_recv.at[(away - 1) * len(cuts) + piece],
            device_id=device_of(1),
            device_id_type=MESH,
        )

    for piece, cut in enumerate(cuts):
        for away in range(1, shards):
            source = (my_shard + shards - away) % shards
            arriving = pltpu.make_async_remote_copy(
                src_ref=hidden.at[:, pl.ds(*cut)],
                dst_ref=hid.at[span(source, core), pl.ds(*cut)],
                send_sem=hid_send.at[away - 1],
                recv_sem=hid_recv.at[(away - 1) * len(cuts) + piece],
                device_id={"shard": source},
                device_id_type=MESH,
            )
            with jax.named_scope(f"x{piece}"):
                arriving.wait_recv()
            relay(source, core, away, piece).start()
            with jax.named_scope(f"f{piece}"):
                forward(source, core, [cut], (away - 1) * 2)
            with jax.named_scope(f"r{piece}"):
                relay(source, 1 - core, away, piece).wait_recv()
            with jax.named_scope(f"g{piece}"):
                forward(source, 1 - core, [cut], (away - 1) * 2 + 1)

    def sides(mask, group):
        return {bit: 1 - mine[bit] if mask >> bit & 1 else mine[bit] for bit in group}

    def remote(source, landing, send, recv, mask):
        return pltpu.make_async_remote_copy(
            src_ref=source,
            dst_ref=landing,
            send_sem=send,
            recv_sem=recv,
            device_id=device_of(mask),
            device_id_type=MESH,
        )

    outer = mine[2] == mine[3]
    inner = mine[2] != mine[3]
    stages, scatter_sems, gather_sems = [], {}, {}
    for chunk, (scatter, gather) in enumerate(routes):
        open_bits, out, into, level, found = list(range(1, bits)), 0, 0, 0, []
        for stage, group in enumerate(scatter):
            gone = [2, 3] if group[0] in (LINE, ACROSS) else group
            after = [bit for bit in open_bits if bit not in gone]
            size = 2 ** len(after)
            if group[0] == LINE:
                pieces, kept = {"far": 2, "near": 1}, 3
            elif group[0] == ACROSS:
                pieces, kept = {8: 1, 12: 1}, 0
            else:
                pieces, kept = {mask: 1 for mask in masks_of(group)[1:]}, 1
            info = {"before": open_bits, "after": after, "size": size, "level": level, "out": {}, "into": {}}
            for name, count in pieces.items():
                info["out"][name] = out
                info["into"][name] = into
                out += count * size
                into += count * size if group[0] != ACROSS else 0
            if group[0] == ACROSS:
                into += size
                info["level"] = found[-1]["level"]
            info["last"] = into
            names = ("far", "near") if group[0] == LINE else ("all",)
            for name in names:
                scatter_sems[chunk, stage, name] = len(scatter_sems)
            level += kept * size
            open_bits = after
            found.append(info)
        stages.append(found)
        for stage, group in enumerate(gather):
            for mask in masks_in(group)[:1] if group[0] == ACROSS else masks_in(group):
                gather_sems[chunk, stage, mask] = len(gather_sems)

    def scatter_copy(chunk, stage, name, mask, begin, into, size):
        return remote(
            sends.at[chunk, pl.ds(begin, size)],
            gots.at[chunk, pl.ds(into, size)],
            rs_send.at[0],
            rs_recv.at[scatter_sems[chunk, stage, name]],
            mask,
        )

    def scatter_send(chunk, stage, mask, name="all", slot=None, count=1):
        info = stages[chunk][stage]
        slot = mask if slot is None else slot
        scatter_copy(chunk, stage, name, mask, info["out"][slot], info["into"][slot], count * info["size"]).start()

    def scatter_wait(chunk, stage, name="all"):
        info, group = stages[chunk][stage], routes[chunk][0][stage]
        if group[0] == LINE:
            first, size = info["into"][name], info["size"] * (2 if name == "far" else 1)
        else:
            first = min(info["into"].values())
            size = info["last"] - first
        scatter_copy(chunk, stage, name, 4, 0, first, size).wait_recv()

    def landed(chunk, stage, index):
        info = stages[chunk][stage]
        total = prod[chunk, info["level"] + index]
        slots = sorted(set(info["into"].values()))
        if routes[chunk][0][stage][0] == ACROSS:
            slots = slots + [stages[chunk][stage - 1]["into"]["near"]]
        for slot in slots:
            total = total + gots[chunk, slot + index].astype(jnp.float32)
        return total

    def hand_out(chunk, stage, blocks_for):
        info, group = stages[chunk][stage], routes[chunk][0][stage]
        size = info["size"]

        def put(mask, bits_of, slot):
            sends[chunk, pl.ds(slot, size)] = blocks_for(mask, bits_of).astype(jnp.bfloat16)

        if group[0] != LINE:
            for mask in reversed(masks_of(group)):
                if mask:
                    put(mask, group, info["out"][mask])
                    scatter_send(chunk, stage, mask)
                else:
                    prod[chunk, pl.ds(info["level"], size)] = blocks_for(0, group)
            return
        far, near = info["out"]["far"], info["out"]["near"]

        @pl.when(outer)
        def _():
            put(12, [2, 3], far)
            put(8, [2, 3], far + size)
            scatter_send(chunk, stage, 4, "far", "far", 2)

        put(4, [2, 3], near)
        scatter_send(chunk, stage, 4, "near", "near")
        prod[chunk, pl.ds(info["level"], size)] = blocks_for(0, [2, 3])

        @pl.when(inner)
        def _():
            prod[chunk, pl.ds(info["level"] + size, size)] = blocks_for(8, [2, 3])
            prod[chunk, pl.ds(info["level"] + 2 * size, size)] = blocks_for(12, [2, 3])

    def backward(lead):
        both = (lead, lead ^ 1)
        columns = pl.ds(lead // 2 * 2 * CHUNK, 2 * CHUNK)

        def product(rows):
            return jnp.dot(
                rows.reshape(-1, joined.shape[-1]), hid[:, columns], preferred_element_type=jnp.float32
            ).reshape(*rows.shape[:-1], 2 * CHUNK)

        def part_of(total, chunk):
            return total[..., chunk % 2 * CHUNK : (chunk % 2 + 1) * CHUNK]

        if all(routes[chunk][0][0] == [1] for chunk in both):
            for mask in (2, 0):
                total = product(joined[:, :, sides(mask, [1])[1]])
                for chunk in both:
                    info = stages[chunk][0]
                    part = part_of(total, chunk).reshape(-1, tall, CHUNK)
                    if mask:
                        sends[chunk, pl.ds(info["out"][mask], info["size"])] = part.astype(jnp.bfloat16)
                        scatter_send(chunk, 0, mask)
                    else:
                        prod[chunk, pl.ds(info["level"], info["size"])] = part
            return
        total = product(joined[...])
        for chunk in both:

            def blocks_for(mask, group, chunk=chunk):
                part = part_of(total, chunk)
                for bit in sorted(group):
                    axis = bits - 1 - bit
                    low, high = (lax.index_in_dim(part, value, axis) for value in range(2))
                    part = jnp.where((mine[bit] == 0) == (mask >> bit & 1 == 0), low, high)
                return part.reshape(-1, tall, CHUNK)

            hand_out(chunk, 0, blocks_for)

    def fold(chunk, stage):
        info, group = stages[chunk][stage], routes[chunk][0][stage]
        size = info["size"]
        if group[0] == ACROSS:

            @pl.when(inner)
            def _():
                scatter_wait(chunk, stage - 1, "far")
                line = stages[chunk][stage - 1]
                for mask, kept, slot in ((8, size, 0), (12, 2 * size, size)):
                    held = prod[chunk, pl.ds(line["level"] + kept, size)]
                    came = gots[chunk, pl.ds(line["into"]["far"] + slot, size)].astype(jnp.float32)
                    sends[chunk, pl.ds(info["out"][mask], size)] = (held + came).astype(jnp.bfloat16)
                    scatter_send(chunk, stage, mask)

            return

        def blocks_for(mask, group):
            found = []
            for spot in range(size):
                values = sides(mask, group)
                values.update({bit: spot // 2**i % 2 for i, bit in enumerate(info["after"])})
                index = sum(values[bit] * 2**i for i, bit in enumerate(info["before"]))
                found.append(landed(chunk, stage - 1, index))
            return jnp.stack(found)

        hand_out(chunk, stage, blocks_for)

    def step_rows(chunk):
        first_fix = 1.0 - beta_one**OPT_STEP
        second_fix = 1.0 - beta_two**OPT_STEP
        here = tuple(reversed(mine))
        sums = landed(chunk, len(routes[chunk][0]) - 1, 0) * scaling
        fresh = []
        for part in range(CHUNK // 128):
            total = sums[:, part * 128 : (part + 1) * 128]
            rows = pl.ds(chunk * (CHUNK // 128) + part, per, stride=width // 128)
            first = beta_one * m_in[rows, :] + (1.0 - beta_one) * total[:per]
            second = beta_two * v_in[rows, :] + (1.0 - beta_two) * total[per:] * total[per:]
            m_out[rows, :] = first
            v_out[rows, :] = second
            update = first / first_fix / (jnp.sqrt(second / second_fix) + epsilon)
            weight = stacked[me // 2, :, pl.ds(chunk * CHUNK + part * 128, 128)].astype(jnp.float32)[:per]
            fresh.append(weight - learn_rate * update)
        half = len(fresh) // 2
        for part in range(half):
            both = jnp.concatenate([fresh[part], fresh[half + part]], axis=0)
            packs[(chunk, *here, slice(None), pl.ds(part * 128, 128))] = both.astype(jnp.bfloat16)

    def gathered(chunk, stage, mask):
        gather = routes[chunk][1]
        have = [bit for group in gather[:stage] for bit in (group if group[0] < LINE else [group[0] - 2])]
        values = sides(mask, range(bits))
        return packs.at[(chunk, *(slice(None) if bit in have else values[bit] for bit in reversed(range(bits))))]

    def gather_start(chunk, stage):
        group = routes[chunk][1][stage]
        where = gathered(chunk, stage, 0)
        if group[0] == ACROSS:
            sem = ag_recv.at[gather_sems[chunk, stage, 8]]

            @pl.when(inner)
            def _():
                for mask in (8, 12):
                    remote(where, where, ag_send.at[1], sem, mask).start()

            return
        for mask in reversed(masks_in(group)):
            remote(where, where, ag_send.at[0], ag_recv.at[gather_sems[chunk, stage, mask]], mask).start()

    def gather_wait(chunk, stage):
        group = routes[chunk][1][stage]
        for mask in [8] if group[0] == ACROSS else masks_in(group):
            where = gathered(chunk, stage, mask)
            remote(where, where, ag_send.at[0], ag_recv.at[gather_sems[chunk, stage, mask]], mask).wait_recv()

    def lay_out(chunk):
        half = CHUNK // 2
        for pair in range(chips):
            spot = tuple(pair // 2**b % 2 for b in reversed(range(bits - 1)))
            even = packs[(chunk, *spot, 0)].astype(jnp.float32)
            odd = packs[(chunk, *spot, 1)].astype(jnp.float32)
            rows = pl.ds(pair * tall, tall)
            for side in range(2):
                part = slice(side * per, (side + 1) * per)
                both = jnp.concatenate([even[part], odd[part]], axis=0)
                w_asm[rows, pl.ds(chunk * CHUNK + side * half, half)] = both.astype(jnp.bfloat16)

    reached = [0] * len(routes)
    for chunk in order:
        scatter, gather = routes[chunk]
        step = reached[chunk]
        if step == 0:
            with jax.named_scope(f"b{chunk // 2}"):
                backward(chunk)
            reached[chunk] = reached[chunk ^ 1] = 1
            continue
        reached[chunk] += 1
        turn = step - len(scatter)
        with jax.named_scope(f"w{chunk}_{step}"):
            if turn <= 0:
                past = scatter[step - 1][0]
                if past == ACROSS:
                    scatter_wait(chunk, step - 2, "near")
                if past != LINE:
                    scatter_wait(chunk, step - 1)
            else:
                gather_wait(chunk, turn - 1)
        with jax.named_scope(f"k{chunk}_{step}"):
            if turn < 0:
                fold(chunk, step)
            elif turn == 0:
                step_rows(chunk)
            if 0 <= turn < len(gather):
                gather_start(chunk, turn)
            elif turn == len(gather):
                lay_out(chunk)
    assert all(done == len(a) + len(b) + 1 for done, (a, b) in zip(reached, routes))

    with jax.named_scope("ends"):
        for copy in pair_sends:
            copy.wait_send()
        whole = hid.at[span(my_shard, core)]
        for away in range(1, shards):
            remote(hidden, whole, hid_send.at[away - 1], hid_recv.at[0], 1).wait_send()
            remote(whole, whole, fwd_send.at[away - 1], fwd_recv.at[0], 1).wait_send()
        flat = sends.reshape(-1, *sends.shape[2:]).at[pl.ds(0, len(routes) * (chips - 1))]
        remote(flat, flat, rs_send.at[0], rs_recv.at[0], 1).wait_send()
        flat = packs.reshape(-1, *packs.shape[-2:])
        plain = across = 0
        for _, gather in routes:
            have = 1
            for group in gather:
                if group[0] == ACROSS:
                    across += 2 * have
                else:
                    plain += have * len(masks_in(group))
                have *= len(masks_of(group)) if group[0] < LINE else 2
        part = flat.at[pl.ds(0, plain)]
        remote(part, part, ag_send.at[0], ag_recv.at[0], 1).wait_send()
        if across:

            @pl.when(inner)
            def _():
                part = flat.at[pl.ds(0, across)]
                remote(part, part, ag_send.at[1], ag_recv.at[0], 1).wait_send()


def copy_out(*refs):
    sources, results, sems = refs[:3], refs[3:6], refs[6]
    copies = [pltpu.make_async_copy(a, b, sems.at[i]) for i, (a, b) in enumerate(zip(sources, results))]
    for copy in copies:
        copy.start()
    for copy in copies:
        copy.wait()


def write_out(results):
    return pl.pallas_call(
        copy_out,
        out_shape=tuple(jax.ShapeDtypeStruct(r.shape, r.dtype) for r in results),
        in_specs=[pl.BlockSpec(memory_space=pl.ANY)] * 3,
        out_specs=(pl.BlockSpec(memory_space=pl.ANY),) * 3,
        scratch_shapes=[pltpu.SemaphoreType.DMA((3,))],
        compiler_params=pltpu.CompilerParams(vmem_limit_bytes=1024 * 1024, has_side_effects=True),
    )(*results)


def in_one_kernel(hidden, resid, target, w_out, signs, m_old, v_old):
    blocks, shards = lax.axis_size("dp"), lax.axis_size("shard")
    features, width = w_out.shape
    tokens = hidden.shape[0]
    per = features // blocks
    tall = 2 * per
    chips = blocks // 2
    bits = blocks.bit_length() - 1
    chunks = width // CHUNK
    routes = routes_of()
    waits = sum(1 if group[0] >= LINE else len(masks_in(group)) for _, gather in routes for group in gather)
    lands = sum(2 if group[0] == LINE else 1 for scatter, _ in routes for group in scatter)
    half = width // 2
    cuts = [(0, half), (half, half - 2 * CHUNK), (width - 2 * CHUNK, CHUNK), (width - CHUNK, CHUNK)]
    scaling = 1.0 / math.sqrt(tokens * blocks * shards)
    bf16, f32 = jnp.bfloat16, jnp.float32
    dma = pltpu.SemaphoreType.DMA
    anywhere = pl.BlockSpec(memory_space=pl.ANY)
    results = pl.pallas_call(
        functools.partial(kernel, routes, ORDER, cuts, scaling),
        out_shape=(
            pltpu.VMEM(w_out.shape, bf16),
            pltpu.VMEM(m_old.shape, f32),
            pltpu.VMEM(v_old.shape, f32),
        ),
        in_specs=[anywhere] * 7,
        out_specs=(pl.BlockSpec(memory_space=pltpu.VMEM),) * 3,
        scratch_shapes=[
            pltpu.VMEM((shards * 2 * tokens, width), bf16),
            pltpu.VMEM((2, *resid.shape), bf16),
            pltpu.VMEM((2, *target.shape), bf16),
            pltpu.VMEM(w_out.shape, bf16),
            pltpu.VMEM(signs.shape, jnp.int32),
            pltpu.VMEM(m_old.shape, f32),
            pltpu.VMEM(v_old.shape, f32),
            pltpu.VMEM((chips, tall, width), bf16),
            pltpu.VMEM((2, chips, per, shards * tokens), f32),
            pltpu.VMEM((*((2,) * (bits - 1)), tall, shards * 2 * tokens), bf16),
            pltpu.VMEM((2 * (shards - 1), chips, tall, tokens), f32),
            pltpu.VMEM((chunks, chips, tall, CHUNK), f32),
            pltpu.VMEM((chunks, chips + 3, tall, CHUNK), bf16),
            pltpu.VMEM((chunks, chips + 1, tall, CHUNK), bf16),
            pltpu.VMEM((chunks, *((2,) * bits), tall, CHUNK // 2), bf16),
            dma((7,)),
            dma((3,)),
            dma((3,)),
            dma((shards - 1,)),
            dma(((shards - 1) * len(cuts),)),
            dma((shards - 1,)),
            dma(((shards - 1) * len(cuts),)),
            dma((1,)),
            dma((lands,)),
            dma((2,)),
            dma((waits,)),
        ],
        compiler_params=pltpu.CompilerParams(
            collective_id=0, has_side_effects=True, vmem_limit_bytes=54 * 1024 * 1024
        ),
    )(hidden, resid, target, w_out, signs, m_old, v_old)
    return write_out(results)


def fits(hidden, w_out):
    blocks, shards = lax.axis_size("dp"), lax.axis_size("shard")
    features, width = w_out.shape
    per = features // blocks
    return (
        shards > 1
        and blocks == 16
        and features % (blocks * 8) == 0
        and features % math.lcm(32, 2 * per) == 0
        and width == len(ROUTES) * CHUNK
        and len(ROUTES) % 2 == 0
        and hidden.shape[0] % 128 == 0
    )


def either(hidden, resid, target, w_out, signs, m_old, v_old):
    run = in_one_kernel if fits(hidden, w_out) else on_device
    return run(hidden, resid, target, w_out, signs, m_old, v_old)


def solution(mesh):
    return jax.shard_map(
        either,
        mesh=mesh,
        in_specs=(
            P(("dp", "shard"), None),
            P("shard", "dp"),
            P("shard", "dp"),
            P("shard", None),
            P("shard", None),
            P(("shard", "dp"), None),
            P(("shard", "dp"), None),
        ),
        out_specs=(P("shard", None), P(("shard", "dp"), None), P(("shard", "dp"), None)),
        check_vma=False,
    )
```
